128 devices in a mesh: bx: 8 (over y, x_hi), by: 16 (over x_lo, z, core).
Axes of the slice: x: 4 (x_hi: 2, x_lo: 2; x = x_hi * 2 + x_lo), y: 4, z: 4, core: 2. Of those that a mesh axis runs over, the one named last changes fastest.
Arguments:
- speed_vectors: float32 [3, 6, 120, 240, 128], P(None, None, 'bx', 'by'), may hold values from -10 to 10, as said below
- bin_population: int32 [120, 240, 128], P('bx', 'by'), may hold values from 0 to 6, as said below
- spin_choice: int32 [12, 120, 240, 128], P(None, 'bx', 'by'), may hold values from 0 to 5
- approval_flags: int32 [12, 120, 240, 128], P(None, 'bx', 'by'), may hold values 0 or 1
- round_evenness: int32 [12], replicated, may hold values from 0 to 1
- grid_displacements: int32 [12], replicated, may hold values from 0 to 127
- thermostat_heat_level: float32 [12], replicated, may hold values from 0.5 to 2
Outputs:
- final_velocity: float32 [3, 6, 120, 240, 128], P(None, None, 'bx', 'by')
The draws below stay inside these ranges and needn't reach their ends.
Inputs may be any that keep to these rules, and one draw needn't show every extreme that they name: `bin_population`: A cell's particles fill its first slots. `speed_vectors`: entries in slots at or beyond a cell's occupancy are not read.
All inputs are finite; a program needn't handle non-finite values. No bound on the sum of `approval_flags` on one device may be relied on, other than what follows from the above.
Results may differ from the reference program's by a relative error of at most 0.0003.
Values sent between devices are 32-bit elements; how exact they have to be, the bound alone decides.
No kernel may reach another device: no remote copies, remote signals or barrier semaphores. Data moves between devices by JAX's collectives and lax.ppermute only.
A program may use at most 64 MiB of HBM per device.

```python
import math
import jax
import jax.numpy as jnp
from jax import lax

SLOTS = 6
NZ = 128
ROUNDS = 6
ENCOUNTER_ROUNDS = 12
NX = 120
NY = 240


def draw_speed_vectors(key, part):
    key_noise, key_rough, key_flow = jax.random.split(jax.random.fold_in(key, 11), 3)
    shape = (3, SLOTS, NX, NY, NZ)
    xgrid = (jnp.arange(NX, dtype=jnp.float32) + 0.5) / NX
    ygrid = (jnp.arange(NY, dtype=jnp.float32) + 0.5) / NY
    rough = jax.random.uniform(key_rough, (NX, NY, NZ), jnp.float32, 0.5, 1.5)
    flowing = 0.7 * jax.random.normal(key_flow, (3, 1, NX, NY, NZ), jnp.float32)
    noise = jax.random.normal(key_noise, shape, jnp.float32)
    profile = (0.6 + 1.2 * xgrid)[:, None, None] + 0.0 * ygrid[None, :, None]
    values = noise * (profile * rough)[None, None] + flowing
    return jnp.clip(values, -10.0, 10.0).astype(jnp.float32)


def draw_bin_population(key, part):
    xgrid = jnp.arange(NX, dtype=jnp.int32)
    banded = (5 * xgrid // NX)[:, None, None]
    return jax.random.randint(jax.random.fold_in(key, 23), (NX, NY, NZ), banded, banded + 3).astype(jnp.int32)


def with_ends(array, key, low, top_value):
    extent = array.shape
    place = [jax.random.randint(jax.random.fold_in(key, axis), (), 0, extent[axis]) for axis in range(len(extent))]
    array = array.at[tuple(place)].set(low)
    longest = extent.index(max(extent))
    place[longest] = (place[longest] + 1) % extent[longest]
    return array.at[tuple(place)].set(top_value)


def setup_inputs(seed: int = 0) -> dict:
    key_list = jax.random.split(jax.random.key(seed), 8)
    speed_vectors = draw_speed_vectors(jax.random.fold_in(key_list[7], 71), 0)
    bin_population = draw_bin_population(jax.random.fold_in(key_list[7], 71), 0)
    spin_choice = with_ends(jax.random.randint(key_list[2], (ENCOUNTER_ROUNDS, NX, NY, NZ), 0, 6), jax.random.fold_in(key_list[2], 1), 0, 5).astype(jnp.int32)
    approval_flags = with_ends((jax.random.randint(key_list[3], (ENCOUNTER_ROUNDS, NX, NY, NZ), 0, 2) < 1).astype(jnp.int32), jax.random.fold_in(key_list[3], 1), 0, 1)
    round_evenness = with_ends(jax.random.randint(key_list[4], (ENCOUNTER_ROUNDS,), 0, 2), jax.random.fold_in(key_list[4], 1), 0, 1).astype(jnp.int32)
    grid_displacements = with_ends(jax.random.randint(key_list[5], (ENCOUNTER_ROUNDS,), 0, NZ), jax.random.fold_in(key_list[5], 1), 0, NZ - 1).astype(jnp.int32)
    thermostat_heat_level = jnp.clip(jnp.exp(jax.random.uniform(key_list[6], (ENCOUNTER_ROUNDS,), jnp.float32, math.log(0.5), math.log(2.0))), 0.5, 2.0)
    return {"speed_vectors": speed_vectors, "bin_population": bin_population, "spin_choice": spin_choice, "approval_flags": approval_flags, "round_evenness": round_evenness, "grid_displacements": grid_displacements, "thermostat_heat_level": thermostat_heat_level}


turn_angle = 130.0 * math.pi / 180.0
drag_gain = 1.0
excess_coupling = 1e-06

def rotate(thermal, spin_choice):
    picked = spin_choice // 2
    unit_axis = [(picked == member).astype(jnp.float32)[None] for member in range(3)]
    sine_term = (math.sin(turn_angle) * (1 - 2 * (spin_choice % 2)).astype(jnp.float32))[None]
    cosine_term = math.cos(turn_angle)
    along_axis = unit_axis[0] * thermal[0] + unit_axis[1] * thermal[1] + unit_axis[2] * thermal[2]
    result = []
    for member in range(3):
        second = (member + 1) % 3
        third_idx = (member + 2) % 3
        cross_term = unit_axis[second] * thermal[third_idx] - unit_axis[third_idx] * thermal[second]
        result.append(cosine_term * thermal[member] + (1.0 - cosine_term) * unit_axis[member] * along_axis + sine_term * cross_term)
    return jnp.stack(result)

def partner_of(values, is_lower, partner_heading):
    return jnp.where(is_lower, jnp.roll(values, -1, partner_heading), jnp.roll(values, 1, partner_heading))

def scatter_bins(speed_vectors, bin_tallies, spin_choice, approval_flags, round_evenness, thermostat_heat_level, overall_work_sum, partner_heading):
    slot_rank = lax.broadcasted_iota(jnp.int32, (speed_vectors.shape[1],) + bin_tallies.shape, 0)
    occupied = (slot_rank < bin_tallies[None]).astype(jnp.float32)
    moment = lax.optimization_barrier(jnp.sum(speed_vectors * occupied[None], axis=1))
    cell_mass = bin_tallies.astype(jnp.float32)
    safe_mass = jnp.maximum(cell_mass, 1.0)
    thermal = (speed_vectors - (moment / safe_mass)[:, None]) * occupied[None]
    accept_bits = approval_flags.astype(jnp.float32)
    coords = lax.broadcasted_iota(jnp.int32, bin_tallies.shape, partner_heading)
    is_lower = (coords - round_evenness) % 2 == 0
    along_moment = moment[partner_heading]
    other_mass = partner_of(cell_mass, is_lower, partner_heading)
    other_moment = partner_of(along_moment, is_lower, partner_heading)
    other_bits = partner_of(accept_bits, is_lower, partner_heading)
    own_speed = along_moment / safe_mass
    other_speed = other_moment / jnp.maximum(other_mass, 1.0)
    closing = jnp.maximum(jnp.where(is_lower, own_speed - other_speed, other_speed - own_speed), 0.0)
    reduced = cell_mass * other_mass / jnp.maximum(cell_mass + other_mass, 1.0)
    transfer = jnp.maximum(accept_bits, other_bits) * reduced * closing * jnp.tanh(drag_gain * closing)
    new_along = along_moment - jnp.where(is_lower, transfer, -transfer)
    moment = jnp.stack([new_along if member == partner_heading else moment[member] for member in range(3)])
    motion_work_sum = jnp.sum(moment * moment / safe_mass) + jnp.sum(thermal * thermal)
    speed_multiplier = jnp.sqrt(3.0 * thermostat_heat_level * overall_work_sum / (motion_work_sum + excess_coupling))
    return speed_multiplier * ((moment / safe_mass)[:, None] * occupied[None] + rotate(thermal, spin_choice))

def reference(speed_vectors, bin_population, spin_choice, approval_flags, round_evenness, grid_displacements, thermostat_heat_level):
    overall_work_sum = jnp.sum(bin_population.astype(jnp.float32))

    def one_round(round_index, carry):
        ensemble_snapshot, bin_tallies = carry
        for displacement_amount in range(2):
            present_round_number = 2 * round_index + displacement_amount
            ensemble_snapshot = scatter_bins(ensemble_snapshot, bin_tallies, spin_choice[present_round_number], approval_flags[present_round_number], round_evenness[present_round_number], thermostat_heat_level[present_round_number], overall_work_sum, displacement_amount)
            shift_by = grid_displacements[present_round_number]
            ensemble_snapshot = jnp.roll(ensemble_snapshot, shift_by, axis=4)
            bin_tallies = jnp.roll(bin_tallies, shift_by, axis=2)
        return (ensemble_snapshot, bin_tallies)
    ensemble_snapshot, bin_tallies = lax.fori_loop(0, ROUNDS, one_round, (speed_vectors, bin_population))
    return ensemble_snapshot
```

```python
import math

import jax
import jax.numpy as jnp
from jax import lax
from jax.experimental import pallas as pl
from jax.experimental.pallas import tpu as pltpu
from jax.sharding import PartitionSpec as P

STEPS = 12
HALF = STEPS // 2
SLOTS = 6
EXT = 15
PAD = 16
HALO = HALF
FULL = EXT + 2 * HALO
PAIRS = (FULL - 1) // 2
NZ = 128
DEVICES = 128
EDGE_PLANES = 2 * HALO + HALO * (HALO + 1) // 2
FIELDS = 2 + HALF

turn_angle = 130.0 * math.pi / 180.0
excess_coupling = 1e-06
BIG = 2.0**46
SCALE_CAP = 3e38
HALF_TAN = math.tan(turn_angle / 2.0)
TURN_NORM = math.cos(turn_angle / 2.0) ** (2 * STEPS)

VMEM = pl.BlockSpec(memory_space=pltpu.VMEM)
SMEM = pl.BlockSpec(memory_space=pltpu.SMEM)
f32 = jnp.float32


def shape(*dims):
    return jax.ShapeDtypeStruct(dims, f32)


def later_shifts(shift_ref, step):
    total = jnp.int32(0)
    for later in range(step, STEPS):
        total = total + shift_ref[later]
    return lax.rem(total, jnp.int32(NZ))


def edge_offsets():
    table = []
    place = 0
    for field in range(FIELDS):
        planes = HALO if field < 2 else HALO - (field - 2)
        table.append((field, place, planes))
        place += planes
    return table


def prep_kernel(shift_ref, v_ref, count_ref, flag_ref, sx_ref, sy_ref, xlo_ref, xhi_ref, ylo_ref, yhi_ref, uz_ref, base_ref, turn_ref):
    shift = later_shifts(shift_ref, 0)
    zero_row = jnp.zeros((EXT, 1, NZ), f32)
    for field in range(FIELDS):
        sx_ref[field, :, EXT:PAD, :] = zero_row
        turn_ref[field, EXT * PAD : PAD * PAD, :] = jnp.zeros((PAD, NZ), f32)
    uz_ref[:, EXT:PAD, :] = zero_row

    def plane(i, sums):
        thermal, energy_y, total = sums
        counts = count_ref[i]
        mass = counts.astype(f32)
        safe = jnp.maximum(mass, 1.0)
        inverse = 1.0 / safe
        mean = []
        for member in range(3):
            values = [
                jnp.where(counts > slot, v_ref[member, slot, i] * BIG, 0.0) for slot in range(SLOTS)
            ]
            moment = values[0]
            for slot in range(1, SLOTS):
                moment = moment + values[slot]
            middle = moment * inverse
            mean.append(middle)
            for slot in range(SLOTS):
                rest = jnp.where(counts > slot, values[slot] - middle, 0.0)
                thermal = thermal + rest * rest
        thermal = thermal + mass * mean[2] * mean[2]
        energy_y = energy_y + mass * mean[1] * mean[1]
        total = total + mass
        rolled = pltpu.roll(mass, shift, 1)
        sx_ref[0, i, 0:EXT, :] = pltpu.roll(mean[0], shift, 1)
        sx_ref[1, i, 0:EXT, :] = rolled
        uz_ref[i, 0:EXT, :] = pltpu.roll(mean[2], shift, 1)
        row = pl.multiple_of(i * PAD, PAD)
        turn_ref[0, pl.ds(row, EXT), :] = pltpu.roll(mean[1], shift, 1)
        turn_ref[1, pl.ds(row, EXT), :] = rolled
        return thermal, energy_y, total

    nothing = jnp.zeros((EXT, NZ), f32)
    thermal, energy_y, total = lax.fori_loop(0, EXT, plane, (nothing, nothing, nothing))
    base_ref[...] = jnp.zeros((8, NZ), f32)
    base_ref[0:1, :] = jnp.full((1, NZ), 1.0 / BIG, f32)
    base_ref[2:3, :] = jnp.sum(thermal, axis=0, keepdims=True)
    base_ref[4:5, :] = jnp.sum(energy_y, axis=0, keepdims=True)
    base_ref[5:6, :] = jnp.sum(total, axis=0, keepdims=True)

    for step in range(STEPS):
        later = later_shifts(shift_ref, step)
        field = 2 + step // 2

        def flags(i, carry, step=step, later=later, field=field):
            bits = pltpu.roll(flag_ref[step, i].astype(f32), later, 1)
            if step % 2 == 0:
                sx_ref[field, i, 0:EXT, :] = bits
            else:
                row = pl.multiple_of(i * PAD, PAD)
                turn_ref[field, pl.ds(row, EXT), :] = bits
            return carry

        lax.fori_loop(0, EXT, flags, 0)

    keep = lax.broadcasted_iota(jnp.int32, (PAD, NZ), 0) < EXT
    for field in range(FIELDS):
        for y in range(EXT):
            rows = turn_ref[field, pl.ds(y, PAD, stride=PAD), :]
            sy_ref[field, y] = jnp.where(keep, rows, 0.0)

    for field, place, planes in edge_offsets():
        for k in range(planes):
            xlo_ref[place + k] = sx_ref[field, k]
            xhi_ref[place + k] = sx_ref[field, EXT - planes + k]
            ylo_ref[place + k] = sy_ref[field, k]
            yhi_ref[place + k] = sy_ref[field, EXT - planes + k]


def prep(shifts, v, counts, flags):
    edge = shape(EDGE_PLANES, PAD, NZ)
    own = shape(FIELDS, EXT, PAD, NZ)
    return pl.pallas_call(
        prep_kernel,
        in_specs=[SMEM, VMEM, VMEM, VMEM],
        out_specs=[VMEM] * 8,
        out_shape=[own, own, edge, edge, edge, edge, shape(EXT, PAD, NZ), shape(8, NZ)],
        scratch_shapes=[pltpu.VMEM((FIELDS, PAD * PAD, NZ), f32)],
        name="prep",
    )(shifts, v, counts, flags)


def lower_start(parity_ref, step, brick_axis):
    return lax.rem(parity_ref[step] + lax.axis_index(brick_axis) * EXT, jnp.int32(2))


def join_kernel(parity_ref, own_ref, below_ref, above_ref, u_ref, *rest, first_step, brick_axis):
    weight_refs, (mass_ref, bits_ref) = rest[:HALF], rest[HALF:]
    for field, place, planes in edge_offsets():
        for k in range(planes):
            low, high = below_ref[place + k], above_ref[place + k]
            if field == 0:
                u_ref[HALO - planes + k] = low
                u_ref[HALO + EXT + k] = high
            elif field == 1:
                mass_ref[HALO - planes + k] = low
                mass_ref[HALO + EXT + k] = high
            else:
                bits_ref[field - 2, HALO - planes + k] = low
                bits_ref[field - 2, HALO + EXT + k] = high
        for k in range(HALO - planes):
            bits_ref[field - 2, k] = jnp.zeros((PAD, NZ), f32)
            bits_ref[field - 2, FULL - 1 - k] = jnp.zeros((PAD, NZ), f32)
    for k in range(EXT):
        u_ref[HALO + k] = own_ref[0, k]
        mass_ref[HALO + k] = own_ref[1, k]
        for j in range(HALF):
            bits_ref[j, HALO + k] = own_ref[2 + j, k]
    for j in range(HALF):
        start = lower_start(parity_ref, first_step + 2 * j, brick_axis)
        for k in range(PAIRS):
            plane = start + 2 * k
            mass_low, mass_high = mass_ref[plane], mass_ref[plane + 1]
            allowed = jnp.maximum(bits_ref[j, plane], bits_ref[j, plane + 1])
            reduced = allowed * mass_low * mass_high / jnp.maximum(mass_low + mass_high, 1.0)
            weight_refs[j][0, k] = reduced / jnp.maximum(mass_low, 1.0)
            weight_refs[j][1, k] = reduced / jnp.maximum(mass_high, 1.0)


def join(parity, own, below, above, first_step, brick_axis):
    def body(*refs):
        join_kernel(*refs, first_step=first_step, brick_axis=brick_axis)

    return pl.pallas_call(
        body,
        in_specs=[SMEM, VMEM, VMEM, VMEM],
        out_specs=[VMEM] * (1 + HALF),
        out_shape=[shape(FULL, PAD, NZ)] + [shape(2, PAIRS, PAD, NZ)] * HALF,
        scratch_shapes=[pltpu.VMEM((FULL, PAD, NZ), f32), pltpu.VMEM((HALF, FULL, PAD, NZ), f32)],
        name="join",
    )(parity, own, below, above)


def next_scale(received_ref, carry_ref, heat_ref, step):
    sums = jnp.sum(received_ref[...], axis=0, keepdims=True)
    scale = carry_ref[0:1, :]
    if step == 0:
        lane = lax.broadcasted_iota(jnp.int32, (1, NZ), 1)
        energy = jnp.sum(jnp.where(lane < NZ // 2, sums, 0.0), axis=1, keepdims=True)
        total = jnp.sum(jnp.where(lane < NZ // 2, 0.0, sums), axis=1, keepdims=True)
        total = jnp.broadcast_to(total, (1, NZ))
    else:
        energy = jnp.sum(sums, axis=1, keepdims=True)
        total = carry_ref[1:2, :]
    speed = scale * jnp.sqrt(jnp.broadcast_to(energy, (1, NZ)))
    factor = jnp.sqrt(3.0 * heat_ref[step] * total / (speed * speed + excess_coupling))
    return jnp.minimum(scale * factor, SCALE_CAP), total


def step_kernel(*refs, step, brick_axis):
    if step == 0:
        parity_ref, carry_ref, u_in_ref, weight_ref, own_ref, u_ref, rows_ref, out_ref = refs
        scale, total = carry_ref[0:1, :], jnp.zeros((1, NZ), f32)
    else:
        parity_ref, heat_ref, received_ref, carry_ref, u_in_ref, weight_ref, own_ref, u_ref, rows_ref, out_ref = refs
        scale, total = next_scale(received_ref, carry_ref, heat_ref, step - 1)
    wide = jnp.broadcast_to(scale, (PAD, NZ))
    start = lower_start(parity_ref, step, brick_axis)
    u_ref[0] = u_in_ref[0]
    u_ref[FULL - 1] = u_in_ref[FULL - 1]
    for k in range(PAIRS):
        plane = start + 2 * k
        low, high = u_in_ref[plane], u_in_ref[plane + 1]
        closing = jnp.maximum(low - high, 0.0)
        push = closing * jnp.tanh(wide * closing)
        u_ref[plane] = low - weight_ref[0, k] * push
        u_ref[plane + 1] = high + weight_ref[1, k] * push
    energy = jnp.zeros((PAD, NZ), f32)
    for k in range(EXT):
        u = u_ref[HALO + k]
        energy = energy + own_ref[1, k] * u * u
    mine = jnp.sum(energy, axis=0, keepdims=True)
    other = carry_ref[4:5, :] if step % 2 == 0 else carry_ref[3:4, :]
    local = carry_ref[2:3, :] + mine + other
    if step == 0:
        half = NZ // 2
        lane = lax.broadcasted_iota(jnp.int32, (1, NZ), 1)
        number = carry_ref[5:6, :]
        local = local + pltpu.roll(local, half, 1)
        number = number + pltpu.roll(number, half, 1)
        local = jnp.where(lane < half, local, number)
    out_ref[...] = carry_ref[...]
    out_ref[0:1, :] = scale
    out_ref[1:2, :] = total
    row = 3 if step % 2 == 0 else 4
    out_ref[row : row + 1, :] = mine
    rows_ref[...] = jnp.broadcast_to(local, (DEVICES, NZ))


def collide(step, parity, heat, received, carry, u, weight, own):
    brick_axis = "bx" if step % 2 == 0 else "by"

    def body(*refs):
        step_kernel(*refs, step=step, brick_axis=brick_axis)

    scalars = (parity,) if step == 0 else (parity, heat)
    arrays = (carry, u, weight, own) if step == 0 else (received, carry, u, weight, own)
    return pl.pallas_call(
        body,
        in_specs=[SMEM] * len(scalars) + [VMEM] * len(arrays),
        out_specs=[VMEM] * 3,
        out_shape=[shape(FULL, PAD, NZ), shape(DEVICES, NZ), shape(8, NZ)],
        name="collide",
    )(*scalars, *arrays)


def turn_kernel(shift_ref, v_ref, count_ref, spin_ref, w_ref):
    shifts = [later_shifts(shift_ref, step) for step in range(STEPS)]

    def plane(i, carry):
        real = jnp.ones((EXT, NZ), f32)
        parts = [jnp.zeros((EXT, NZ), f32)] * 3
        for step in range(STEPS):
            spin = pltpu.roll(spin_ref[step, i], shifts[step], 1)
            tangent = jnp.where((spin & 1) == 0, HALF_TAN, -HALF_TAN)
            on_x, on_y = spin < 2, spin < 4
            x, y, z = parts

            def pick(first, second, third):
                return tangent * jnp.where(on_x, first, jnp.where(on_y, second, third))

            real, parts = (
                real - pick(x, y, z),
                [x + pick(real, z, -y), y + pick(-z, real, x), z + pick(y, -x, real)],
            )
        x, y, z = parts
        unit = BIG * TURN_NORM
        xx, yy, zz, rr = x * x, y * y, z * z, real * real
        rows = [
            [(rr + xx) - (yy + zz), 2.0 * (x * y - real * z), 2.0 * (x * z + real * y)],
            [2.0 * (x * y + real * z), (rr + yy) - (xx + zz), 2.0 * (y * z - real * x)],
            [2.0 * (x * z - real * y), 2.0 * (y * z + real * x), (rr + zz) - (xx + yy)],
        ]
        rows = [[unit * value for value in row] for row in rows]
        counts = pltpu.roll(count_ref[i], shifts[0], 1)
        inverse = 1.0 / jnp.maximum(counts.astype(f32), 1.0)
        values = [
            [
                jnp.where(counts > slot, pltpu.roll(v_ref[member, slot, i], shifts[0], 1), 0.0)
                for slot in range(SLOTS)
            ]
            for member in range(3)
        ]
        mean = []
        for member in range(3):
            moment = values[member][0]
            for slot in range(1, SLOTS):
                moment = moment + values[member][slot]
            mean.append(moment * inverse)
        for slot in range(SLOTS):
            rest = [values[member][slot] - mean[member] for member in range(3)]
            for member in range(3):
                turned = rows[member][0] * rest[0] + rows[member][1] * rest[1] + rows[member][2] * rest[2]
                w_ref[member, slot, i] = turned
        return carry

    lax.fori_loop(0, EXT, plane, 0)


def turn(shifts, v, counts, spin):
    return pl.pallas_call(
        turn_kernel,
        in_specs=[SMEM, VMEM, VMEM, VMEM],
        out_specs=VMEM,
        out_shape=shape(3, SLOTS, EXT, EXT, NZ),
        name="turn",
    )(shifts, v, counts, spin)


def finish_kernel(heat_ref, received_ref, carry_ref, ux_ref, uy_ref, uz_ref, own_ref, w_ref, v_ref):
    scale, _ = next_scale(received_ref, carry_ref, heat_ref, STEPS - 1)
    wide = jnp.broadcast_to(scale, (EXT, NZ))
    for i in range(EXT):
        counts = own_ref[1, i, 0:EXT, :]
        mean = [
            ux_ref[HALO + i, 0:EXT, :],
            uy_ref[pl.ds(HALO * PAD + i, EXT, stride=PAD), :],
            uz_ref[i, 0:EXT, :],
        ]
        for member in range(3):
            for slot in range(SLOTS):
                value = wide * (mean[member] + w_ref[member, slot, i])
                v_ref[member, slot, i] = jnp.where(counts > slot, value, 0.0)


def finish(heat, received, carry, ux, uy, uz, own, w):
    return pl.pallas_call(
        finish_kernel,
        in_specs=[SMEM] + [VMEM] * 7,
        out_specs=VMEM,
        out_shape=shape(3, SLOTS, EXT, EXT, NZ),
        name="finish",
    )(heat, received, carry, ux, uy.reshape(FULL * PAD, NZ), uz, own, w)


def exchange(low_edge, high_edge, axis):
    count = lax.axis_size(axis)
    down = [(source, (source - 1) % count) for source in range(count)]
    up = [(source, (source + 1) % count) for source in range(count)]
    return lax.ppermute(low_edge, axis, down), lax.ppermute(high_edge, axis, up)


def per_device(v, counts, spin, flags, parity, shifts, heat):
    sx, sy, xlo, xhi, ylo, yhi, uz, carry = prep(shifts, v, counts, flags)
    x_above, x_below = exchange(xlo, xhi, "bx")
    y_above, y_below = exchange(ylo, yhi, "by")
    w = turn(shifts, v, counts, spin)
    ux, *x_weights = join(parity, sx, x_below, x_above, 0, "bx")
    uy, *y_weights = join(parity, sy, y_below, y_above, 1, "by")
    received = None
    for step in range(STEPS):
        if step % 2 == 0:
            ux, rows, carry = collide(step, parity, heat, received, carry, ux, x_weights[step // 2], sx)
        else:
            uy, rows, carry = collide(step, parity, heat, received, carry, uy, y_weights[step // 2], sy)
        received = lax.all_to_all(rows, ("bx", "by"), 0, 0, tiled=True)
    return finish(heat, received, carry, ux, uy, uz, sx, w)


def solution(mesh):
    return jax.shard_map(
        per_device,
        mesh=mesh,
        in_specs=(
            P(None, None, "bx", "by", None),
            P("bx", "by", None),
            P(None, "bx", "by", None),
            P(None, "bx", "by", None),
            P(),
            P(),
            P(),
        ),
        out_specs=P(None, None, "bx", "by", None),
        check_vma=False,
    )
```

```python
import math

import jax
import jax.numpy as jnp
from jax import lax
from jax.experimental import pallas as pl
from jax.experimental.pallas import tpu as pltpu
from jax.sharding import PartitionSpec as P

STEPS = 12
HALF = STEPS // 2
SLOTS = 6
EXT = 15
PAD = 16
HALO = HALF
FULL = EXT + 2 * HALO
PAIRS = (FULL - 1) // 2
NZ = 128
DEVICES = 128
EDGE_PLANES = 2 * HALO + HALO * (HALO + 1) // 2
FIELDS = 2 + HALF

turn_angle = 130.0 * math.pi / 180.0
excess_coupling = 1e-06
BIG = 2.0**46
SCALE_CAP = 3e38
HALF_TAN = math.tan(turn_angle / 2.0)
TURN_NORM = math.cos(turn_angle / 2.0) ** (2 * STEPS)

VMEM = pl.BlockSpec(memory_space=pltpu.VMEM)
SMEM = pl.BlockSpec(memory_space=pltpu.SMEM)
f32 = jnp.float32
GRANT = pltpu.CompilerParams(vmem_limit_bytes=12 * 2**20)


def shape(*dims):
    return jax.ShapeDtypeStruct(dims, f32)


def later_shifts(shift_ref, step):
    total = jnp.int32(0)
    for later in range(step, STEPS):
        total = total + shift_ref[later]
    return lax.rem(total, jnp.int32(NZ))


def edge_offsets():
    table = []
    place = 0
    for field in range(FIELDS):
        planes = HALO if field < 2 else HALO - (field - 2)
        table.append((field, place, planes))
        place += planes
    return table


def fold(values):
    return jnp.sum(values, axis=0, keepdims=True)


def prep_kernel(
    shift_ref, v_ref, count_ref, flag_hbm, own_ref, uy_ref, uz_ref, low_ref, high_ref, base_ref, flag_ref, flag_sem
):
    fetch = pltpu.make_async_copy(flag_hbm.at[0], flag_ref, flag_sem)
    fetch.start()
    shift = later_shifts(shift_ref, 0)
    zero_row = jnp.zeros((EXT, 1, NZ), f32)
    for field in range(3):
        own_ref[field, :, EXT:PAD, :] = zero_row
    for array_ref in (uy_ref, uz_ref):
        array_ref[0:EXT, EXT:PAD, :] = zero_row
    uy_ref[EXT] = jnp.zeros((PAD, NZ), f32)

    thermal = energy_y = total = jnp.zeros((EXT, NZ), f32)
    fetch.wait()
    for i in range(EXT):
        counts = count_ref[i]
        mass = counts.astype(f32)
        inverse = 1.0 / jnp.maximum(mass, 1.0)
        mean = []
        for member in range(3):
            values = [
                jnp.where(counts > slot, v_ref[member, slot, i] * BIG, 0.0) for slot in range(SLOTS)
            ]
            moment = values[0]
            for slot in range(1, SLOTS):
                moment = moment + values[slot]
            middle = moment * inverse
            mean.append(middle)
            for slot in range(SLOTS):
                rest = jnp.where(counts > slot, values[slot] - middle, 0.0)
                thermal = thermal + rest * rest
        thermal = thermal + mass * mean[2] * mean[2]
        energy_y = energy_y + mass * mean[1] * mean[1]
        total = total + mass
        own_ref[0, i, 0:EXT, :] = pltpu.roll(mean[0], shift, 1)
        own_ref[1, i, 0:EXT, :] = pltpu.roll(mass, shift, 1)
        own_ref[2, i, 0:EXT, :] = pltpu.roll(flag_ref[i].astype(f32), shift, 1)
        uy_ref[i, 0:EXT, :] = pltpu.roll(mean[1], shift, 1)
        uz_ref[i, 0:EXT, :] = pltpu.roll(mean[2], shift, 1)
    base_ref[...] = jnp.zeros((8, NZ), f32)
    base_ref[0:1, :] = jnp.full((1, NZ), 1.0 / BIG, f32)
    base_ref[2:3, :] = fold(thermal)
    base_ref[4:5, :] = fold(energy_y)
    base_ref[5:6, :] = fold(total)
    for field in range(3):
        low_ref[field] = own_ref[field, 0]
        high_ref[field] = own_ref[field, EXT - 1]


def prep(shifts, v, counts, flags):
    edge = shape(3, PAD, NZ)
    return pl.pallas_call(
        prep_kernel,
        in_specs=[SMEM, VMEM, VMEM, pl.BlockSpec(memory_space=pl.ANY)],
        out_specs=[VMEM] * 6,
        out_shape=[shape(3, EXT, PAD, NZ), shape(PAD, PAD, NZ), shape(EXT, PAD, NZ), edge, edge, shape(8, NZ)],
        scratch_shapes=[pltpu.VMEM((EXT, EXT, NZ), jnp.int32), pltpu.SemaphoreType.DMA],
        compiler_params=GRANT,
        name="prep",
    )(shifts, v, counts, flags)


def spread_kernel(shift_ref, own_ref, uy_ref, flag_ref, sx_ref, sy_ref, xlo_ref, xhi_ref, ylo_ref, yhi_ref, turn_ref):
    for field in range(HALF):
        sx_ref[2 + field, :, EXT:PAD, :] = jnp.zeros((EXT, 1, NZ), f32)
    for i in range(EXT):
        sx_ref[0, i] = own_ref[0, i]
        sx_ref[1, i] = own_ref[1, i]
    for step in range(STEPS):
        later = later_shifts(shift_ref, step)
        for i in range(EXT):
            bits = pltpu.roll(flag_ref[step, i].astype(f32), later, 1)
            if step % 2 == 0:
                sx_ref[2 + step // 2, i, 0:EXT, :] = bits
            else:
                turn_ref[step // 2, i * PAD : i * PAD + EXT, :] = bits
    keep = lax.broadcasted_iota(jnp.int32, (PAD, NZ), 0) < EXT
    for i in range(EXT):
        turn_ref[HALF, i * PAD : (i + 1) * PAD, :] = own_ref[1, i]
    for field in range(FIELDS):
        for y in range(EXT):
            if field == 0:
                rows = uy_ref[pl.ds(y, PAD, stride=PAD), :]
            else:
                rows = turn_ref[HALF if field == 1 else field - 2, pl.ds(y, PAD, stride=PAD), :]
            sy_ref[field, y] = jnp.where(keep, rows, 0.0)

    for field, place, planes in edge_offsets():
        for k in range(planes):
            xlo_ref[place + k] = sx_ref[field, k]
            xhi_ref[place + k] = sx_ref[field, EXT - planes + k]
            ylo_ref[place + k] = sy_ref[field, k]
            yhi_ref[place + k] = sy_ref[field, EXT - planes + k]


def spread(shifts, own, uy, flags):
    edge = shape(EDGE_PLANES, PAD, NZ)
    full = shape(FIELDS, EXT, PAD, NZ)
    return pl.pallas_call(
        spread_kernel,
        in_specs=[SMEM, VMEM, VMEM, VMEM],
        out_specs=[VMEM] * 6,
        out_shape=[full, full, edge, edge, edge, edge],
        scratch_shapes=[pltpu.VMEM((HALF + 1, PAD * PAD, NZ), f32)],
        compiler_params=GRANT,
        name="spread",
    )(shifts, own, uy.reshape(PAD * PAD, NZ), flags)


def first_kernel(parity_ref, own_ref, below_ref, above_ref, carry_ref, rows_ref, out_ref, u_ref, mass_ref, bits_ref):
    for field, array_ref in enumerate((u_ref, mass_ref, bits_ref)):
        array_ref[0] = below_ref[field]
        array_ref[EXT + 1] = above_ref[field]
        for k in range(EXT):
            array_ref[1 + k] = own_ref[field, k]
    start = lax.rem(lower_start(parity_ref, 0, "bx") + 1, jnp.int32(2))
    wide = jnp.broadcast_to(carry_ref[0:1, :], (PAD, NZ))
    for k in range((EXT + 1) // 2):
        plane = start + 2 * k
        low, high = u_ref[plane], u_ref[plane + 1]
        weight_low, weight_high = pair_weights(mass_ref[plane], mass_ref[plane + 1])
        allowed = jnp.maximum(bits_ref[plane], bits_ref[plane + 1])
        closing = jnp.maximum(low - high, 0.0)
        push = allowed * closing * jnp.tanh(wide * closing)
        u_ref[plane] = low - weight_low * push
        u_ref[plane + 1] = high + weight_high * push
    energy = jnp.zeros((PAD, NZ), f32)
    for k in range(EXT):
        u = u_ref[1 + k]
        energy = energy + own_ref[1, k] * u * u
    mine = fold(energy)
    half = NZ // 2
    lane = lax.broadcasted_iota(jnp.int32, (1, NZ), 1)
    local = carry_ref[2:3, :] + mine + carry_ref[4:5, :]
    number = carry_ref[5:6, :]
    local = jnp.where(lane < half, local + pltpu.roll(local, half, 1), number + pltpu.roll(number, half, 1))
    out_ref[...] = carry_ref[...]
    out_ref[3:4, :] = mine
    rows_ref[...] = jnp.broadcast_to(local, (DEVICES, NZ))


def first(parity, own, below, above, carry):
    return pl.pallas_call(
        first_kernel,
        in_specs=[SMEM] + [VMEM] * 4,
        out_specs=[VMEM] * 2,
        out_shape=[shape(DEVICES, NZ), shape(8, NZ)],
        scratch_shapes=[pltpu.VMEM((EXT + 2, PAD, NZ), f32)] * 3,
        compiler_params=GRANT,
        name="first",
    )(parity, own, below, above, carry)


def lower_start(parity_ref, step, brick_axis):
    return lax.rem(parity_ref[step] + lax.axis_index(brick_axis) * EXT, jnp.int32(2))


def pair_weights(mass_low, mass_high):
    reduced = mass_low * mass_high / jnp.maximum(mass_low + mass_high, 1.0)
    return reduced / jnp.maximum(mass_low, 1.0), reduced / jnp.maximum(mass_high, 1.0)


def pairs_step(u_ref, weight_ref, start, wide):
    for k in range(PAIRS):
        plane = start + 2 * k
        low, high = u_ref[plane], u_ref[plane + 1]
        closing = jnp.maximum(low - high, 0.0)
        push = closing * jnp.tanh(wide * closing)
        u_ref[plane] = low - weight_ref[0, k] * push
        u_ref[plane + 1] = high + weight_ref[1, k] * push


def join_kernel(parity_ref, own_ref, below_ref, above_ref, u_ref, *rest, first_step, brick_axis):
    weight_refs, (own_mass_ref, mass_ref, bits_ref, both_ref) = rest[:HALF], rest[HALF:]
    for field, place, planes in edge_offsets():
        for k in range(planes):
            low, high = below_ref[place + k], above_ref[place + k]
            if field == 0:
                u_ref[HALO - planes + k] = low
                u_ref[HALO + EXT + k] = high
            elif field == 1:
                mass_ref[HALO - planes + k] = low
                mass_ref[HALO + EXT + k] = high
            else:
                bits_ref[field - 2, HALO - planes + k] = low
                bits_ref[field - 2, HALO + EXT + k] = high
        for k in range(HALO - planes):
            bits_ref[field - 2, k] = jnp.zeros((PAD, NZ), f32)
            bits_ref[field - 2, FULL - 1 - k] = jnp.zeros((PAD, NZ), f32)
    for k in range(EXT):
        u_ref[HALO + k] = own_ref[0, k]
        mass_ref[HALO + k] = own_ref[1, k]
        own_mass_ref[k] = own_ref[1, k]
        for j in range(HALF):
            bits_ref[j, HALO + k] = own_ref[2 + j, k]
    for plane in range(FULL - 1):
        both_ref[0, plane], both_ref[1, plane] = pair_weights(mass_ref[plane], mass_ref[plane + 1])
    for j in range(HALF):
        start = lower_start(parity_ref, first_step + 2 * j, brick_axis)
        for k in range(PAIRS):
            plane = start + 2 * k
            allowed = jnp.maximum(bits_ref[j, plane], bits_ref[j, plane + 1])
            weight_refs[j][0, k] = allowed * both_ref[0, plane]
            weight_refs[j][1, k] = allowed * both_ref[1, plane]
    if first_step == 0:
        start = lower_start(parity_ref, 0, brick_axis)
        pairs_step(u_ref, weight_refs[0], start, jnp.full((PAD, NZ), 1.0 / BIG, f32))


def join(parity, own, below, above, first_step, brick_axis):
    def body(*refs):
        join_kernel(*refs, first_step=first_step, brick_axis=brick_axis)

    return pl.pallas_call(
        body,
        in_specs=[SMEM, VMEM, VMEM, VMEM],
        out_specs=[VMEM] * (2 + HALF),
        out_shape=[shape(FULL, PAD, NZ)] + [shape(2, PAIRS, PAD, NZ)] * HALF + [shape(EXT, PAD, NZ)],
        scratch_shapes=[
            pltpu.VMEM((FULL, PAD, NZ), f32),
            pltpu.VMEM((HALF, FULL, PAD, NZ), f32),
            pltpu.VMEM((2, FULL, PAD, NZ), f32),
        ],
        compiler_params=GRANT,
        name="join",
    )(parity, own, below, above)


def next_scale(received_ref, carry_ref, heat_ref, step):
    sums = jnp.sum(received_ref[...], axis=0, keepdims=True)
    scale = carry_ref[0:1, :]
    if step == 0:
        lane = lax.broadcasted_iota(jnp.int32, (1, NZ), 1)
        energy = jnp.sum(jnp.where(lane < NZ // 2, sums, 0.0), axis=1, keepdims=True)
        total = jnp.sum(jnp.where(lane < NZ // 2, 0.0, sums), axis=1, keepdims=True)
        total = jnp.broadcast_to(total, (1, NZ))
    else:
        energy = jnp.sum(sums, axis=1, keepdims=True)
        total = carry_ref[1:2, :]
    speed = scale * jnp.sqrt(jnp.broadcast_to(energy, (1, NZ)))
    factor = jnp.sqrt(3.0 * heat_ref[step] * total / (speed * speed + excess_coupling))
    return jnp.minimum(scale * factor, SCALE_CAP), total


def step_kernel(
    parity_ref, heat_ref, received_ref, carry_ref, u_in_ref, weight_ref, mass_ref, u_ref, rows_ref, out_ref, *, step, brick_axis
):
    scale, total = next_scale(received_ref, carry_ref, heat_ref, step - 1)
    start = lower_start(parity_ref, step, brick_axis)
    for k in range(FULL):
        u_ref[k] = u_in_ref[k]
    pairs_step(u_ref, weight_ref, start, jnp.broadcast_to(scale, (PAD, NZ)))
    energy = jnp.zeros((PAD, NZ), f32)
    for k in range(EXT):
        u = u_ref[HALO + k]
        energy = energy + mass_ref[k] * u * u
    mine = fold(energy)
    other = carry_ref[4:5, :] if step % 2 == 0 else carry_ref[3:4, :]
    out_ref[...] = carry_ref[...]
    out_ref[0:1, :] = scale
    out_ref[1:2, :] = total
    row = 3 if step % 2 == 0 else 4
    out_ref[row : row + 1, :] = mine
    rows_ref[...] = jnp.broadcast_to(carry_ref[2:3, :] + mine + other, (DEVICES, NZ))


def collide(step, parity, heat, received, carry, u, weight, mass):
    brick_axis = "bx" if step % 2 == 0 else "by"

    def body(*refs):
        step_kernel(*refs, step=step, brick_axis=brick_axis)

    return pl.pallas_call(
        body,
        in_specs=[SMEM] * 2 + [VMEM] * 5,
        out_specs=[VMEM] * 3,
        out_shape=[shape(FULL, PAD, NZ), shape(DEVICES, NZ), shape(8, NZ)],
        compiler_params=GRANT,
        name="collide",
    )(parity, heat, received, carry, u, weight, mass)


def turn_kernel(shift_ref, v_ref, count_ref, spin_ref, w_ref):
    shifts = [later_shifts(shift_ref, step) for step in range(STEPS)]

    def plane(i, carry):
        real = jnp.ones((EXT, NZ), f32)
        parts = [jnp.zeros((EXT, NZ), f32)] * 3
        for step in range(STEPS):
            spin = pltpu.roll(spin_ref[step, i], shifts[step], 1)
            tangent = jnp.where((spin & 1) == 0, HALF_TAN, -HALF_TAN)
            on_x, on_y = spin < 2, spin < 4
            x, y, z = parts

            def pick(first, second, third):
                return tangent * jnp.where(on_x, first, jnp.where(on_y, second, third))

            real, parts = (
                real - pick(x, y, z),
                [x + pick(real, z, -y), y + pick(-z, real, x), z + pick(y, -x, real)],
            )
        x, y, z = parts
        unit = BIG * TURN_NORM
        xx, yy, zz, rr = x * x, y * y, z * z, real * real
        rows = [
            [(rr + xx) - (yy + zz), 2.0 * (x * y - real * z), 2.0 * (x * z + real * y)],
            [2.0 * (x * y + real * z), (rr + yy) - (xx + zz), 2.0 * (y * z - real * x)],
            [2.0 * (x * z - real * y), 2.0 * (y * z + real * x), (rr + zz) - (xx + yy)],
        ]
        rows = [[unit * value for value in row] for row in rows]
        counts = pltpu.roll(count_ref[i], shifts[0], 1)
        inverse = 1.0 / jnp.maximum(counts.astype(f32), 1.0)
        values = [
            [
                jnp.where(counts > slot, pltpu.roll(v_ref[member, slot, i], shifts[0], 1), 0.0)
                for slot in range(SLOTS)
            ]
            for member in range(3)
        ]
        mean = []
        for member in range(3):
            moment = values[member][0]
            for slot in range(1, SLOTS):
                moment = moment + values[member][slot]
            mean.append(moment * inverse)
        for slot in range(SLOTS):
            rest = [values[member][slot] - mean[member] for member in range(3)]
            for member in range(3):
                turned = rows[member][0] * rest[0] + rows[member][1] * rest[1] + rows[member][2] * rest[2]
                w_ref[member, slot, i] = turned
        return carry

    lax.fori_loop(0, EXT, plane, 0)


def turn(shifts, v, counts, spin):
    return pl.pallas_call(
        turn_kernel,
        in_specs=[SMEM, VMEM, VMEM, VMEM],
        out_specs=VMEM,
        out_shape=shape(3, SLOTS, EXT, EXT, NZ),
        compiler_params=GRANT,
        name="turn",
    )(shifts, v, counts, spin)


def finish_kernel(heat_ref, received_ref, carry_ref, ux_ref, uy_ref, uz_ref, own_ref, w_ref, v_ref):
    member = pl.program_id(0)
    scale, _ = next_scale(received_ref, carry_ref, heat_ref, STEPS - 1)
    wide = jnp.broadcast_to(scale, (EXT, NZ))

    def write(mean_of):
        for i in range(EXT):
            counts = own_ref[0, i, 0:EXT, :]
            mean = mean_of(i)
            for slot in range(SLOTS):
                v_ref[0, slot, i] = jnp.where(counts > slot, wide * (mean + w_ref[0, slot, i]), 0.0)

    @pl.when(member == 0)
    def _():
        write(lambda i: ux_ref[HALO + i, 0:EXT, :])

    @pl.when(member == 1)
    def _():
        write(lambda i: uy_ref[pl.ds(HALO * PAD + i, EXT, stride=PAD), :])

    @pl.when(member == 2)
    def _():
        write(lambda i: uz_ref[i, 0:EXT, :])


def finish(heat, received, carry, ux, uy, uz, own, w):
    part = pl.BlockSpec((1, SLOTS, EXT, EXT, NZ), lambda c: (c, 0, 0, 0, 0))
    mass = pl.BlockSpec((1, EXT, PAD, NZ), lambda c: (1, 0, 0, 0))
    return pl.pallas_call(
        finish_kernel,
        grid=(3,),
        in_specs=[SMEM] + [VMEM] * 5 + [mass, part],
        out_specs=part,
        out_shape=shape(3, SLOTS, EXT, EXT, NZ),
        compiler_params=GRANT,
        name="finish",
    )(heat, received, carry, ux, uy.reshape(FULL * PAD, NZ), uz, own, w)


def exchange(low_edge, high_edge, axis):
    count = lax.axis_size(axis)
    down = [(source, (source - 1) % count) for source in range(count)]
    up = [(source, (source + 1) % count) for source in range(count)]
    return lax.ppermute(low_edge, axis, down), lax.ppermute(high_edge, axis, up)


def per_device(v, counts, spin, flags, parity, shifts, heat):
    own, uy, uz, low, high, carry = prep(shifts, v, counts, flags)
    above, below = exchange(low, high, "bx")
    sx, sy, xlo, xhi, ylo, yhi = spread(shifts, own, uy, flags)
    y_above, y_below = exchange(ylo, yhi, "by")
    x_above, x_below = exchange(xlo, xhi, "bx")
    rows, carry = first(parity, own, below, above, carry)
    received = lax.all_to_all(rows, ("bx", "by"), 0, 0, tiled=True)
    w = turn(shifts, v, counts, spin)
    uy, *y_weights, y_mass = join(parity, sy, y_below, y_above, 1, "by")
    ux, *x_weights, x_mass = join(parity, sx, x_below, x_above, 0, "bx")
    for step in range(1, STEPS):
        if step % 2 == 0:
            ux, rows, carry = collide(step, parity, heat, received, carry, ux, x_weights[step // 2], x_mass)
        else:
            uy, rows, carry = collide(step, parity, heat, received, carry, uy, y_weights[step // 2], y_mass)
        received = lax.all_to_all(rows, ("bx", "by"), 0, 0, tiled=True)
    return finish(heat, received, carry, ux, uy, uz, own, w)


def solution(mesh):
    return jax.shard_map(
        per_device,
        mesh=mesh,
        in_specs=(
            P(None, None, "bx", "by", None),
            P("bx", "by", None),
            P(None, "bx", "by", None),
            P(None, "bx", "by", None),
            P(),
            P(),
            P(),
        ),
        out_specs=P(None, None, "bx", "by", None),
        check_vma=False,
    )
```

```python
import math

import jax
import jax.numpy as jnp
from jax import lax
from jax.experimental import pallas as pl
from jax.experimental.pallas import tpu as pltpu
from jax.sharding import PartitionSpec as P

STEPS = 12
HALF = STEPS // 2
SLOTS = 6
EXT = 15
PAD = 16
CHUNK = 3
NZ = 128
DEVICES = 128
X_LEFT = HALF - 1
Y_LEFT = HALF

turn_angle = 130.0 * math.pi / 180.0
excess_coupling = 1e-06
BIG = 2.0**46
SCALE_CAP = 3e38
HALF_TAN = math.tan(turn_angle / 2.0)
TURN_NORM = math.cos(turn_angle / 2.0) ** (2 * STEPS)

VMEM = pl.BlockSpec(memory_space=pltpu.VMEM)
SMEM = pl.BlockSpec(memory_space=pltpu.SMEM)
ANY = pl.BlockSpec(memory_space=pl.ANY)
f32 = jnp.float32
GRANT = pltpu.CompilerParams(vmem_limit_bytes=12 * 2**20)


def shape(*dims):
    return jax.ShapeDtypeStruct(dims, f32)


def later_shifts(shift_ref, step):
    total = jnp.int32(0)
    for later in range(step, STEPS):
        total = total + shift_ref[later]
    return lax.rem(total, jnp.int32(NZ))


def edge_layout(left):
    counts = [left, left] + [left - k for k in range(left)]
    starts = [sum(counts[:k]) for k in range(len(counts))]
    return list(zip(starts, counts)), sum(counts)


def full_planes(left):
    return EXT + 2 * left


def pair_count(left):
    return (full_planes(left) - 1) // 2


def fold(values):
    return jnp.sum(values, axis=0, keepdims=True)


def prep_kernel(
    shift_hbm, v_hbm, count_hbm, flag_hbm, own_ref, uy_ref, uz_ref, low_ref, high_ref, base_ref,
    shift_ref, v_ref, count_ref, flag_ref, sems, chunk_sems,
):
    fetches = [
        pltpu.make_async_copy(shift_hbm, shift_ref, sems.at[0]),
        pltpu.make_async_copy(count_hbm, count_ref, sems.at[1]),
        pltpu.make_async_copy(flag_hbm.at[0], flag_ref, sems.at[2]),
    ]
    chunks = [
        pltpu.make_async_copy(
            v_hbm.at[:, :, pl.ds(CHUNK * c, CHUNK)], v_ref.at[:, :, pl.ds(CHUNK * c, CHUNK)], chunk_sems.at[c]
        )
        for c in range(EXT // CHUNK)
    ]
    for fetch in fetches + chunks:
        fetch.start()
    for fetch in fetches:
        fetch.wait()
    shift = later_shifts(shift_ref, 0)
    zero_row = jnp.zeros((EXT, 1, NZ), f32)
    for field in range(3):
        own_ref[field, :, EXT:PAD, :] = zero_row
    for array_ref in (uy_ref, uz_ref):
        array_ref[0:EXT, EXT:PAD, :] = zero_row
    uy_ref[EXT] = jnp.zeros((PAD, NZ), f32)

    thermal = energy_y = total = jnp.zeros((EXT, NZ), f32)
    for i in range(EXT):
        if i % CHUNK == 0:
            chunks[i // CHUNK].wait()
        counts = count_ref[i]
        mass = counts.astype(f32)
        inverse = 1.0 / jnp.maximum(mass, 1.0)
        mean = []
        for member in range(3):
            values = [
                jnp.where(counts > slot, v_ref[member, slot, i] * BIG, 0.0) for slot in range(SLOTS)
            ]
            moment = values[0]
            for slot in range(1, SLOTS):
                moment = moment + values[slot]
            middle = moment * inverse
            mean.append(middle)
            for slot in range(SLOTS):
                rest = jnp.where(counts > slot, values[slot] - middle, 0.0)
                thermal = thermal + rest * rest
        thermal = thermal + mass * mean[2] * mean[2]
        energy_y = energy_y + mass * mean[1] * mean[1]
        total = total + mass
        own_ref[0, i, 0:EXT, :] = pltpu.roll(mean[0], shift, 1)
        own_ref[1, i, 0:EXT, :] = pltpu.roll(mass, shift, 1)
        own_ref[2, i, 0:EXT, :] = pltpu.roll(flag_ref[i].astype(f32), shift, 1)
        uy_ref[i, 0:EXT, :] = pltpu.roll(mean[1], shift, 1)
        uz_ref[i, 0:EXT, :] = pltpu.roll(mean[2], shift, 1)
    base_ref[...] = jnp.zeros((8, NZ), f32)
    base_ref[0:1, :] = jnp.full((1, NZ), 1.0 / BIG, f32)
    base_ref[2:3, :] = fold(thermal)
    base_ref[4:5, :] = fold(energy_y)
    base_ref[5:6, :] = fold(total)
    for field in range(3):
        low_ref[field] = own_ref[field, 0]
        high_ref[field] = own_ref[field, EXT - 1]


def prep(shifts, v, counts, flags):
    edge = shape(3, PAD, NZ)
    return pl.pallas_call(
        prep_kernel,
        in_specs=[ANY] * 4,
        out_specs=[VMEM] * 6,
        out_shape=[shape(3, EXT, PAD, NZ), shape(PAD, PAD, NZ), shape(EXT, PAD, NZ), edge, edge, shape(8, NZ)],
        scratch_shapes=[
            pltpu.SMEM((STEPS,), jnp.int32),
            pltpu.VMEM((3, SLOTS, EXT, EXT, NZ), f32),
            pltpu.VMEM((EXT, EXT, NZ), jnp.int32),
            pltpu.VMEM((EXT, EXT, NZ), jnp.int32),
            pltpu.SemaphoreType.DMA((3,)),
            pltpu.SemaphoreType.DMA((EXT // CHUNK,)),
        ],
        compiler_params=GRANT,
        name="prep",
    )(*[pltpu.with_memory_space_constraint(array, pltpu.HBM) for array in (shifts, v, counts, flags)])


def spread_kernel(shift_ref, own_ref, uy_ref, flag_ref, bits_ref, sy_ref, low_ref, high_ref, turn_ref):
    bits_ref[:, :, EXT:PAD, :] = jnp.zeros((X_LEFT, EXT, 1, NZ), f32)
    for step in range(1, STEPS):
        later = later_shifts(shift_ref, step)
        for i in range(EXT):
            bits = pltpu.roll(flag_ref[step, i].astype(f32), later, 1)
            if step % 2 == 0:
                bits_ref[step // 2 - 1, i, 0:EXT, :] = bits
            else:
                turn_ref[step // 2, i * PAD : i * PAD + EXT, :] = bits
    keep = lax.broadcasted_iota(jnp.int32, (PAD, NZ), 0) < EXT
    for i in range(EXT):
        turn_ref[HALF, i * PAD : (i + 1) * PAD, :] = own_ref[1, i]
    for field in range(2 + Y_LEFT):
        for y in range(EXT):
            if field == 0:
                rows = uy_ref[pl.ds(y, PAD, stride=PAD), :]
            else:
                rows = turn_ref[HALF if field == 1 else field - 2, pl.ds(y, PAD, stride=PAD), :]
            sy_ref[field, y] = jnp.where(keep, rows, 0.0)
    for field, (place, planes) in enumerate(edge_layout(Y_LEFT)[0]):
        for k in range(planes):
            low_ref[place + k] = sy_ref[field, k]
            high_ref[place + k] = sy_ref[field, EXT - planes + k]


def spread(shifts, own, uy, flags):
    edge = shape(edge_layout(Y_LEFT)[1], PAD, NZ)
    return pl.pallas_call(
        spread_kernel,
        in_specs=[SMEM, VMEM, VMEM, VMEM],
        out_specs=[VMEM] * 4,
        out_shape=[shape(X_LEFT, EXT, PAD, NZ), shape(2 + Y_LEFT, EXT, PAD, NZ), edge, edge],
        scratch_shapes=[pltpu.VMEM((HALF + 1, PAD * PAD, NZ), f32)],
        compiler_params=GRANT,
        name="spread",
    )(shifts, own, uy.reshape(PAD * PAD, NZ), flags)


def lower_start(parity_ref, step, brick_axis, halo):
    return lax.rem(parity_ref[step] + lax.axis_index(brick_axis) * EXT + halo, jnp.int32(2))


def first_kernel(
    parity_ref, own_ref, bits_ref, below_ref, above_ref, carry_ref,
    rows_ref, out_ref, sx_ref, xlo_ref, xhi_ref, u_ref, mass_ref, allow_ref,
):
    for field, array_ref in enumerate((u_ref, mass_ref, allow_ref)):
        array_ref[0] = below_ref[field]
        array_ref[EXT + 1] = above_ref[field]
        for k in range(EXT):
            array_ref[1 + k] = own_ref[field, k]
    start = lower_start(parity_ref, 0, "bx", 1)
    wide = jnp.broadcast_to(carry_ref[0:1, :], (PAD, NZ))
    for k in range((EXT + 1) // 2):
        plane = start + 2 * k
        low, high = u_ref[plane], u_ref[plane + 1]
        weight_low, weight_high = pair_weights(mass_ref[plane], mass_ref[plane + 1])
        allowed = jnp.maximum(allow_ref[plane], allow_ref[plane + 1])
        closing = jnp.maximum(low - high, 0.0)
        push = allowed * closing * jnp.tanh(wide * closing)
        u_ref[plane] = low - weight_low * push
        u_ref[plane + 1] = high + weight_high * push
    energy = jnp.zeros((PAD, NZ), f32)
    for k in range(EXT):
        u = u_ref[1 + k]
        energy = energy + own_ref[1, k] * u * u
        sx_ref[0, k] = u
        sx_ref[1, k] = own_ref[1, k]
        for j in range(X_LEFT):
            sx_ref[2 + j, k] = bits_ref[j, k]
    for field, (place, planes) in enumerate(edge_layout(X_LEFT)[0]):
        for k in range(planes):
            xlo_ref[place + k] = sx_ref[field, k]
            xhi_ref[place + k] = sx_ref[field, EXT - planes + k]
    mine = fold(energy)
    half = NZ // 2
    lane = lax.broadcasted_iota(jnp.int32, (1, NZ), 1)
    local = carry_ref[2:3, :] + mine + carry_ref[4:5, :]
    number = carry_ref[5:6, :]
    local = jnp.where(lane < half, local + pltpu.roll(local, half, 1), number + pltpu.roll(number, half, 1))
    out_ref[...] = carry_ref[...]
    out_ref[3:4, :] = mine
    rows_ref[...] = jnp.broadcast_to(local, (DEVICES, NZ))


def first(parity, own, bits, below, above, carry):
    edge = shape(edge_layout(X_LEFT)[1], PAD, NZ)
    return pl.pallas_call(
        first_kernel,
        in_specs=[SMEM] + [VMEM] * 5,
        out_specs=[VMEM] * 5,
        out_shape=[shape(DEVICES, NZ), shape(8, NZ), shape(2 + X_LEFT, EXT, PAD, NZ), edge, edge],
        scratch_shapes=[pltpu.VMEM((EXT + 2, PAD, NZ), f32)] * 3,
        compiler_params=GRANT,
        name="first",
    )(parity, own, bits, below, above, carry)


def pair_weights(mass_low, mass_high):
    reduced = mass_low * mass_high / jnp.maximum(mass_low + mass_high, 1.0)
    return reduced / jnp.maximum(mass_low, 1.0), reduced / jnp.maximum(mass_high, 1.0)


def join_kernel(parity_ref, own_ref, below_ref, above_ref, u_ref, weight_ref, mass_ref, all_mass_ref, bits_ref, both_ref, *, left, brick_axis):
    for field, (place, planes) in enumerate(edge_layout(left)[0]):
        for k in range(planes):
            low, high = below_ref[place + k], above_ref[place + k]
            below, above = left - planes + k, left + EXT + k
            if field == 0:
                u_ref[below], u_ref[above] = low, high
            elif field == 1:
                all_mass_ref[below], all_mass_ref[above] = low, high
            else:
                bits_ref[field - 2, below], bits_ref[field - 2, above] = low, high
        for k in range(left - planes):
            bits_ref[field - 2, k] = jnp.zeros((PAD, NZ), f32)
            bits_ref[field - 2, full_planes(left) - 1 - k] = jnp.zeros((PAD, NZ), f32)
    for k in range(EXT):
        u_ref[left + k] = own_ref[0, k]
        all_mass_ref[left + k] = own_ref[1, k]
        mass_ref[k] = own_ref[1, k]
        for j in range(left):
            bits_ref[j, left + k] = own_ref[2 + j, k]
    for plane in range(full_planes(left) - 1):
        both_ref[0, plane], both_ref[1, plane] = pair_weights(all_mass_ref[plane], all_mass_ref[plane + 1])
    for j in range(left):
        step = STEPS - 2 * (left - j) + (0 if brick_axis == "bx" else 1)
        start = lower_start(parity_ref, step, brick_axis, left)
        for k in range(pair_count(left)):
            plane = start + 2 * k
            allowed = jnp.maximum(bits_ref[j, plane], bits_ref[j, plane + 1])
            weight_ref[j, 0, k] = allowed * both_ref[0, plane]
            weight_ref[j, 1, k] = allowed * both_ref[1, plane]


def join(parity, own, below, above, left, brick_axis):
    def body(*refs):
        join_kernel(*refs, left=left, brick_axis=brick_axis)

    full, pairs = full_planes(left), pair_count(left)
    return pl.pallas_call(
        body,
        in_specs=[SMEM, VMEM, VMEM, VMEM],
        out_specs=[VMEM] * 3,
        out_shape=[shape(full, PAD, NZ), shape(left, 2, pairs, PAD, NZ), shape(EXT, PAD, NZ)],
        scratch_shapes=[
            pltpu.VMEM((full, PAD, NZ), f32),
            pltpu.VMEM((left, full, PAD, NZ), f32),
            pltpu.VMEM((2, full, PAD, NZ), f32),
        ],
        compiler_params=GRANT,
        name="join",
    )(parity, own, below, above)


def next_scale(received_ref, carry_ref, heat_ref, step):
    sums = jnp.sum(received_ref[...], axis=0, keepdims=True)
    scale = carry_ref[0:1, :]
    if step == 0:
        lane = lax.broadcasted_iota(jnp.int32, (1, NZ), 1)
        energy = jnp.sum(jnp.where(lane < NZ // 2, sums, 0.0), axis=1, keepdims=True)
        total = jnp.sum(jnp.where(lane < NZ // 2, 0.0, sums), axis=1, keepdims=True)
        total = jnp.broadcast_to(total, (1, NZ))
    else:
        energy = jnp.sum(sums, axis=1, keepdims=True)
        total = carry_ref[1:2, :]
    speed = scale * jnp.sqrt(jnp.broadcast_to(energy, (1, NZ)))
    factor = jnp.sqrt(3.0 * heat_ref[step] * total / (speed * speed + excess_coupling))
    return jnp.minimum(scale * factor, SCALE_CAP), total


def step_kernel(
    parity_ref, heat_ref, received_ref, carry_ref, u_in_ref, weight_ref, mass_ref, u_ref, rows_ref, out_ref, *, step, left, brick_axis
):
    scale, total = next_scale(received_ref, carry_ref, heat_ref, step - 1)
    start = lower_start(parity_ref, step, brick_axis, left)
    wide = jnp.broadcast_to(scale, (PAD, NZ))
    turn = left - (STEPS + 1 - step) // 2
    for k in range(full_planes(left)):
        u_ref[k] = u_in_ref[k]
    for k in range(pair_count(left)):
        plane = start + 2 * k
        low, high = u_ref[plane], u_ref[plane + 1]
        closing = jnp.maximum(low - high, 0.0)
        push = closing * jnp.tanh(wide * closing)
        u_ref[plane] = low - weight_ref[turn, 0, k] * push
        u_ref[plane + 1] = high + weight_ref[turn, 1, k] * push
    energy = jnp.zeros((PAD, NZ), f32)
    for k in range(EXT):
        u = u_ref[left + k]
        energy = energy + mass_ref[k] * u * u
    mine = fold(energy)
    other = carry_ref[4:5, :] if step % 2 == 0 else carry_ref[3:4, :]
    out_ref[...] = carry_ref[...]
    out_ref[0:1, :] = scale
    out_ref[1:2, :] = total
    row = 3 if step % 2 == 0 else 4
    out_ref[row : row + 1, :] = mine
    rows_ref[...] = jnp.broadcast_to(carry_ref[2:3, :] + mine + other, (DEVICES, NZ))


def collide(step, parity, heat, received, carry, u, weight, mass):
    left, brick_axis = (X_LEFT, "bx") if step % 2 == 0 else (Y_LEFT, "by")

    def body(*refs):
        step_kernel(*refs, step=step, left=left, brick_axis=brick_axis)

    return pl.pallas_call(
        body,
        in_specs=[SMEM] * 2 + [VMEM] * 5,
        out_specs=[VMEM] * 3,
        out_shape=[shape(full_planes(left), PAD, NZ), shape(DEVICES, NZ), shape(8, NZ)],
        compiler_params=GRANT,
        name="collide",
    )(parity, heat, received, carry, u, weight, mass)


def turn_kernel(shift_ref, v_ref, count_ref, spin_ref, w_ref):
    shifts = [later_shifts(shift_ref, step) for step in range(STEPS)]

    def plane(i, carry):
        real = jnp.ones((EXT, NZ), f32)
        parts = [jnp.zeros((EXT, NZ), f32)] * 3
        for step in range(STEPS):
            spin = pltpu.roll(spin_ref[step, i], shifts[step], 1)
            tangent = jnp.where((spin & 1) == 0, HALF_TAN, -HALF_TAN)
            on_x, on_y = spin < 2, spin < 4
            x, y, z = parts

            def pick(first, second, third):
                return tangent * jnp.where(on_x, first, jnp.where(on_y, second, third))

            real, parts = (
                real - pick(x, y, z),
                [x + pick(real, z, -y), y + pick(-z, real, x), z + pick(y, -x, real)],
            )
        x, y, z = parts
        unit = BIG * TURN_NORM
        xx, yy, zz, rr = x * x, y * y, z * z, real * real
        rows = [
            [(rr + xx) - (yy + zz), 2.0 * (x * y - real * z), 2.0 * (x * z + real * y)],
            [2.0 * (x * y + real * z), (rr + yy) - (xx + zz), 2.0 * (y * z - real * x)],
            [2.0 * (x * z - real * y), 2.0 * (y * z + real * x), (rr + zz) - (xx + yy)],
        ]
        rows = [[unit * value for value in row] for row in rows]
        counts = pltpu.roll(count_ref[i], shifts[0], 1)
        inverse = 1.0 / jnp.maximum(counts.astype(f32), 1.0)
        values = [
            [
                jnp.where(counts > slot, pltpu.roll(v_ref[member, slot, i], shifts[0], 1), 0.0)
                for slot in range(SLOTS)
            ]
            for member in range(3)
        ]
        mean = []
        for member in range(3):
            moment = values[member][0]
            for slot in range(1, SLOTS):
                moment = moment + values[member][slot]
            mean.append(moment * inverse)
        for slot in range(SLOTS):
            rest = [values[member][slot] - mean[member] for member in range(3)]
            for member in range(3):
                turned = rows[member][0] * rest[0] + rows[member][1] * rest[1] + rows[member][2] * rest[2]
                w_ref[member, slot, i] = turned
        return carry

    lax.fori_loop(0, EXT, plane, 0)


def turn(shifts, v, counts, spin):
    return pl.pallas_call(
        turn_kernel,
        in_specs=[SMEM, VMEM, VMEM, VMEM],
        out_specs=VMEM,
        out_shape=shape(3, SLOTS, EXT, EXT, NZ),
        compiler_params=GRANT,
        name="turn",
    )(shifts, v, counts, spin)


def finish_kernel(heat_ref, received_ref, carry_ref, ux_ref, uy_ref, uz_ref, own_ref, w_ref, v_ref):
    member = pl.program_id(0)
    scale, _ = next_scale(received_ref, carry_ref, heat_ref, STEPS - 1)
    wide = jnp.broadcast_to(scale, (EXT, NZ))

    def write(mean_of):
        for i in range(EXT):
            counts = own_ref[0, i, 0:EXT, :]
            mean = mean_of(i)
            for slot in range(SLOTS):
                v_ref[0, slot, i] = jnp.where(counts > slot, wide * (mean + w_ref[0, slot, i]), 0.0)

    @pl.when(member == 0)
    def _():
        write(lambda i: ux_ref[X_LEFT + i, 0:EXT, :])

    @pl.when(member == 1)
    def _():
        write(lambda i: uy_ref[pl.ds(Y_LEFT * PAD + i, EXT, stride=PAD), :])

    @pl.when(member == 2)
    def _():
        write(lambda i: uz_ref[i, 0:EXT, :])


def finish(heat, received, carry, ux, uy, uz, own, w):
    part = pl.BlockSpec((1, SLOTS, EXT, EXT, NZ), lambda c: (c, 0, 0, 0, 0))
    mass = pl.BlockSpec((1, EXT, PAD, NZ), lambda c: (1, 0, 0, 0))
    return pl.pallas_call(
        finish_kernel,
        grid=(3,),
        in_specs=[SMEM] + [VMEM] * 5 + [mass, part],
        out_specs=part,
        out_shape=shape(3, SLOTS, EXT, EXT, NZ),
        compiler_params=GRANT,
        name="finish",
    )(heat, received, carry, ux, uy.reshape(full_planes(Y_LEFT) * PAD, NZ), uz, own, w)


def exchange(low_edge, high_edge, axis):
    count = lax.axis_size(axis)
    down = [(source, (source - 1) % count) for source in range(count)]
    up = [(source, (source + 1) % count) for source in range(count)]
    return lax.ppermute(low_edge, axis, down), lax.ppermute(high_edge, axis, up)


def sum_over_devices(rows):
    return lax.all_to_all(rows, ("bx", "by"), 0, 0, tiled=True)


def per_device(v, counts, spin, flags, parity, shifts, heat):
    own, uy, uz, low, high, carry = prep(shifts, v, counts, flags)
    above, below = exchange(low, high, "bx")
    bits, sy, ylo, yhi = spread(shifts, own, uy, flags)
    y_above, y_below = exchange(ylo, yhi, "by")
    rows, carry, sx, xlo, xhi = first(parity, own, bits, below, above, carry)
    received = sum_over_devices(rows)
    x_above, x_below = exchange(xlo, xhi, "bx")
    w = turn(shifts, v, counts, spin)
    uy, y_weights, y_mass = join(parity, sy, y_below, y_above, Y_LEFT, "by")
    ux, x_weights, x_mass = join(parity, sx, x_below, x_above, X_LEFT, "bx")
    for step in range(1, STEPS):
        if step % 2 == 0:
            ux, rows, carry = collide(step, parity, heat, received, carry, ux, x_weights, x_mass)
        else:
            uy, rows, carry = collide(step, parity, heat, received, carry, uy, y_weights, y_mass)
        received = sum_over_devices(rows)
    return finish(heat, received, carry, ux, uy, uz, own, w)


def solution(mesh):
    return jax.shard_map(
        per_device,
        mesh=mesh,
        in_specs=(
            P(None, None, "bx", "by", None),
            P("bx", "by", None),
            P(None, "bx", "by", None),
            P(None, "bx", "by", None),
            P(),
            P(),
            P(),
        ),
        out_specs=P(None, None, "bx", "by", None),
        check_vma=False,
    )
```

```python
import math

import jax
import jax.numpy as jnp
from jax import lax
from jax.experimental import pallas as pl
from jax.experimental.pallas import tpu as pltpu
from jax.sharding import PartitionSpec as P

STEPS = 12
HALF = STEPS // 2
SLOTS = 6
EXT = 15
PAD = 16
CHUNK = 3
TURN_STEP = 5
NZ = 128
DEVICES = 128
X_LEFT = HALF - 1
Y_LEFT = HALF
HEAT_ROW = 8
START_ROW = HEAT_ROW + PAD
CARRY = START_ROW + PAD

turn_angle = 130.0 * math.pi / 180.0
excess_coupling = 1e-06
BIG = 2.0**46
SCALE_CAP = 3e38
HALF_TAN = math.tan(turn_angle / 2.0)
TURN_NORM = math.cos(turn_angle / 2.0) ** (2 * STEPS)

VMEM = pl.BlockSpec(memory_space=pltpu.VMEM)
SMEM = pl.BlockSpec(memory_space=pltpu.SMEM)
ANY = pl.BlockSpec(memory_space=pl.ANY)
f32 = jnp.float32
GRANT = pltpu.CompilerParams(vmem_limit_bytes=12 * 2**20)


def shape(*dims):
    return jax.ShapeDtypeStruct(dims, f32)


def later_shifts(shift_ref, step):
    total = jnp.int32(0)
    for later in range(step, STEPS):
        total = total + shift_ref[later]
    return lax.rem(total, jnp.int32(NZ))


def edge_layout(left):
    counts = [left, left] + [left - k for k in range(left)]
    starts = [sum(counts[:k]) for k in range(len(counts))]
    return list(zip(starts, counts)), sum(counts)


def full_planes(left):
    return EXT + 2 * left


def pair_count(left):
    return (full_planes(left) - 1) // 2


def place_of(step):
    return (X_LEFT, "bx") if step % 2 == 0 else (Y_LEFT, "by")


def fold(values):
    return jnp.sum(values, axis=0, keepdims=True)


def prep_kernel(
    shift_hbm, parity_hbm, heat_hbm, v_hbm, count_hbm, flag_hbm, own_ref, uy_ref, uz_ref, low_ref, high_ref, base_ref,
    shift_ref, parity_ref, heat_ref, v_ref, count_ref, flag_ref, sems, chunk_sems,
):
    fetches = [
        pltpu.make_async_copy(shift_hbm, shift_ref, sems.at[0]),
        pltpu.make_async_copy(count_hbm, count_ref, sems.at[1]),
        pltpu.make_async_copy(flag_hbm.at[0], flag_ref, sems.at[2]),
        pltpu.make_async_copy(parity_hbm, parity_ref, sems.at[3]),
        pltpu.make_async_copy(heat_hbm, heat_ref, sems.at[4]),
    ]
    chunks = [
        pltpu.make_async_copy(
            v_hbm.at[:, :, pl.ds(CHUNK * c, CHUNK)], v_ref.at[:, :, pl.ds(CHUNK * c, CHUNK)], chunk_sems.at[c]
        )
        for c in range(EXT // CHUNK)
    ]
    for fetch in fetches + chunks:
        fetch.start()
    for fetch in fetches:
        fetch.wait()
    shift = later_shifts(shift_ref, 0)
    zero_row = jnp.zeros((EXT, 1, NZ), f32)
    for field in range(3):
        own_ref[field, :, EXT:PAD, :] = zero_row
    for array_ref in (uy_ref, uz_ref):
        array_ref[0:EXT, EXT:PAD, :] = zero_row
    uy_ref[EXT] = jnp.zeros((PAD, NZ), f32)

    thermal = energy_y = total = jnp.zeros((EXT, NZ), f32)
    for i in range(EXT):
        if i % CHUNK == 0:
            chunks[i // CHUNK].wait()
        counts = count_ref[i]
        mass = counts.astype(f32)
        inverse = 1.0 / jnp.maximum(mass, 1.0)
        mean = []
        for member in range(3):
            values = [
                jnp.where(counts > slot, v_ref[member, slot, i] * BIG, 0.0) for slot in range(SLOTS)
            ]
            moment = values[0]
            for slot in range(1, SLOTS):
                moment = moment + values[slot]
            middle = moment * inverse
            mean.append(middle)
            for slot in range(SLOTS):
                rest = jnp.where(counts > slot, values[slot] - middle, 0.0)
                thermal = thermal + rest * rest
        thermal = thermal + mass * mean[2] * mean[2]
        energy_y = energy_y + mass * mean[1] * mean[1]
        total = total + mass
        own_ref[0, i, 0:EXT, :] = pltpu.roll(mean[0], shift, 1)
        own_ref[1, i, 0:EXT, :] = pltpu.roll(mass, shift, 1)
        own_ref[2, i, 0:EXT, :] = pltpu.roll(flag_ref[i].astype(f32), shift, 1)
        uy_ref[i, 0:EXT, :] = pltpu.roll(mean[1], shift, 1)
        uz_ref[i, 0:EXT, :] = pltpu.roll(mean[2], shift, 1)
    base_ref[...] = jnp.zeros((CARRY, NZ), f32)
    for step in range(STEPS):
        left, brick_axis = place_of(step)
        start = lower_start(parity_ref, step, brick_axis, left)
        base_ref[HEAT_ROW + step : HEAT_ROW + step + 1, :] = jnp.full((1, NZ), 3.0 * heat_ref[step], f32)
        base_ref[START_ROW + step : START_ROW + step + 1, :] = jnp.full((1, NZ), start.astype(f32), f32)
    base_ref[0:1, :] = jnp.full((1, NZ), 1.0 / BIG, f32)
    base_ref[2:3, :] = fold(thermal)
    base_ref[4:5, :] = fold(energy_y)
    base_ref[5:6, :] = fold(total)
    for field in range(3):
        low_ref[field] = own_ref[field, 0]
        high_ref[field] = own_ref[field, EXT - 1]


def prep(shifts, parity, heat, v, counts, flags):
    edge = shape(3, PAD, NZ)
    return pl.pallas_call(
        prep_kernel,
        in_specs=[ANY] * 6,
        out_specs=[VMEM] * 6,
        out_shape=[shape(3, EXT, PAD, NZ), shape(PAD, PAD, NZ), shape(EXT, PAD, NZ), edge, edge, shape(CARRY, NZ)],
        scratch_shapes=[
            pltpu.SMEM((STEPS,), jnp.int32),
            pltpu.SMEM((STEPS,), jnp.int32),
            pltpu.SMEM((STEPS,), f32),
            pltpu.VMEM((3, SLOTS, EXT, EXT, NZ), f32),
            pltpu.VMEM((EXT, EXT, NZ), jnp.int32),
            pltpu.VMEM((EXT, EXT, NZ), jnp.int32),
            pltpu.SemaphoreType.DMA((5,)),
            pltpu.SemaphoreType.DMA((EXT // CHUNK,)),
        ],
        compiler_params=GRANT,
        name="prep",
    )(*[pltpu.with_memory_space_constraint(array, pltpu.HBM) for array in (shifts, parity, heat, v, counts, flags)])


def spread_kernel(shift_ref, own_ref, uy_ref, flag_ref, bits_ref, sy_ref, low_ref, high_ref, turn_ref):
    bits_ref[:, :, EXT:PAD, :] = jnp.zeros((X_LEFT, EXT, 1, NZ), f32)
    for step in range(1, STEPS):
        later = later_shifts(shift_ref, step)
        for i in range(EXT):
            bits = pltpu.roll(flag_ref[step, i].astype(f32), later, 1)
            if step % 2 == 0:
                bits_ref[step // 2 - 1, i, 0:EXT, :] = bits
            else:
                turn_ref[step // 2, i * PAD : i * PAD + EXT, :] = bits
    keep = lax.broadcasted_iota(jnp.int32, (PAD, NZ), 0) < EXT
    for i in range(EXT):
        turn_ref[HALF, i * PAD : (i + 1) * PAD, :] = own_ref[1, i]
    for field in range(2 + Y_LEFT):
        for y in range(EXT):
            if field == 0:
                rows = uy_ref[pl.ds(y, PAD, stride=PAD), :]
            else:
                rows = turn_ref[HALF if field == 1 else field - 2, pl.ds(y, PAD, stride=PAD), :]
            sy_ref[field, y] = jnp.where(keep, rows, 0.0)
    for field, (place, planes) in enumerate(edge_layout(Y_LEFT)[0]):
        for k in range(planes):
            low_ref[place + k] = sy_ref[field, k]
            high_ref[place + k] = sy_ref[field, EXT - planes + k]


def spread(shifts, own, uy, flags):
    edge = shape(edge_layout(Y_LEFT)[1], PAD, NZ)
    return pl.pallas_call(
        spread_kernel,
        in_specs=[SMEM, VMEM, VMEM, VMEM],
        out_specs=[VMEM] * 4,
        out_shape=[shape(X_LEFT, EXT, PAD, NZ), shape(2 + Y_LEFT, EXT, PAD, NZ), edge, edge],
        scratch_shapes=[pltpu.VMEM((HALF + 1, PAD * PAD, NZ), f32)],
        compiler_params=GRANT,
        name="spread",
    )(shifts, own, uy.reshape(PAD * PAD, NZ), flags)


def lower_start(parity_ref, step, brick_axis, halo):
    return lax.rem(parity_ref[step] + lax.axis_index(brick_axis) * EXT + halo, jnp.int32(2))


def first_kernel(
    parity_ref, own_ref, bits_ref, below_ref, above_ref, carry_ref,
    rows_ref, out_ref, sx_ref, xlo_ref, xhi_ref, u_ref, mass_ref, allow_ref,
):
    for field, array_ref in enumerate((u_ref, mass_ref, allow_ref)):
        array_ref[0] = below_ref[field]
        array_ref[EXT + 1] = above_ref[field]
        for k in range(EXT):
            array_ref[1 + k] = own_ref[field, k]
    start = lower_start(parity_ref, 0, "bx", 1)
    wide = jnp.broadcast_to(carry_ref[0:1, :], (PAD, NZ))
    for k in range((EXT + 1) // 2):
        plane = start + 2 * k
        low, high = u_ref[plane], u_ref[plane + 1]
        weight_low, weight_high = pair_weights(mass_ref[plane], mass_ref[plane + 1])
        allowed = jnp.maximum(allow_ref[plane], allow_ref[plane + 1])
        closing = jnp.maximum(low - high, 0.0)
        push = allowed * closing * jnp.tanh(wide * closing)
        u_ref[plane] = low - weight_low * push
        u_ref[plane + 1] = high + weight_high * push
    energy = jnp.zeros((PAD, NZ), f32)
    for k in range(EXT):
        u = u_ref[1 + k]
        energy = energy + own_ref[1, k] * u * u
        sx_ref[0, k] = u
        sx_ref[1, k] = own_ref[1, k]
        for j in range(X_LEFT):
            sx_ref[2 + j, k] = bits_ref[j, k]
    for field, (place, planes) in enumerate(edge_layout(X_LEFT)[0]):
        for k in range(planes):
            xlo_ref[place + k] = sx_ref[field, k]
            xhi_ref[place + k] = sx_ref[field, EXT - planes + k]
    mine = fold(energy)
    half = NZ // 2
    lane = lax.broadcasted_iota(jnp.int32, (1, NZ), 1)
    local = carry_ref[2:3, :] + mine + carry_ref[4:5, :]
    number = carry_ref[5:6, :]
    local = jnp.where(lane < half, local + pltpu.roll(local, half, 1), number + pltpu.roll(number, half, 1))
    out_ref[...] = carry_ref[...]
    out_ref[3:4, :] = mine
    rows_ref[...] = jnp.broadcast_to(local, (DEVICES, NZ))


def first(parity, own, bits, below, above, carry):
    edge = shape(edge_layout(X_LEFT)[1], PAD, NZ)
    return pl.pallas_call(
        first_kernel,
        in_specs=[SMEM] + [VMEM] * 5,
        out_specs=[VMEM] * 5,
        out_shape=[shape(DEVICES, NZ), shape(CARRY, NZ), shape(2 + X_LEFT, EXT, PAD, NZ), edge, edge],
        scratch_shapes=[pltpu.VMEM((EXT + 2, PAD, NZ), f32)] * 3,
        compiler_params=GRANT,
        name="first",
    )(parity, own, bits, below, above, carry)


def pair_weights(mass_low, mass_high):
    reduced = mass_low * mass_high / jnp.maximum(mass_low + mass_high, 1.0)
    return reduced / jnp.maximum(mass_low, 1.0), reduced / jnp.maximum(mass_high, 1.0)


def join_kernel(parity_ref, own_ref, below_ref, above_ref, u_ref, weight_ref, mass_ref, all_mass_ref, bits_ref, both_ref, *, left, brick_axis):
    for field, (place, planes) in enumerate(edge_layout(left)[0]):
        for k in range(planes):
            low, high = below_ref[place + k], above_ref[place + k]
            below, above = left - planes + k, left + EXT + k
            if field == 0:
                u_ref[below], u_ref[above] = low, high
            elif field == 1:
                all_mass_ref[below], all_mass_ref[above] = low, high
            else:
                bits_ref[field - 2, below], bits_ref[field - 2, above] = low, high
        for k in range(left - planes):
            bits_ref[field - 2, k] = jnp.zeros((PAD, NZ), f32)
            bits_ref[field - 2, full_planes(left) - 1 - k] = jnp.zeros((PAD, NZ), f32)
    for k in range(EXT):
        u_ref[left + k] = own_ref[0, k]
        all_mass_ref[left + k] = own_ref[1, k]
        mass_ref[k] = own_ref[1, k]
        for j in range(left):
            bits_ref[j, left + k] = own_ref[2 + j, k]
    for plane in range(full_planes(left) - 1):
        both_ref[0, plane], both_ref[1, plane] = pair_weights(all_mass_ref[plane], all_mass_ref[plane + 1])
    for j in range(left):
        step = STEPS - 2 * (left - j) + (0 if brick_axis == "bx" else 1)
        start = lower_start(parity_ref, step, brick_axis, left)
        for k in range(pair_count(left)):
            plane = start + 2 * k
            allowed = jnp.maximum(bits_ref[j, plane], bits_ref[j, plane + 1])
            weight_ref[j, 0, k] = allowed * both_ref[0, plane]
            weight_ref[j, 1, k] = allowed * both_ref[1, plane]


def join(parity, own, below, above, left, brick_axis):
    def body(*refs):
        join_kernel(*refs, left=left, brick_axis=brick_axis)

    full, pairs = full_planes(left), pair_count(left)
    return pl.pallas_call(
        body,
        in_specs=[SMEM, VMEM, VMEM, VMEM],
        out_specs=[VMEM] * 3,
        out_shape=[shape(full, PAD, NZ), shape(left, 2, pairs, PAD, NZ), shape(EXT, PAD, NZ)],
        scratch_shapes=[
            pltpu.VMEM((full, PAD, NZ), f32),
            pltpu.VMEM((left, full, PAD, NZ), f32),
            pltpu.VMEM((2, full, PAD, NZ), f32),
        ],
        compiler_params=GRANT,
        name="join",
    )(parity, own, below, above)


def next_scale(received_ref, carry_ref, step):
    sums = jnp.sum(received_ref[...], axis=0, keepdims=True)
    scale = carry_ref[0:1, :]
    if step == 0:
        lane = lax.broadcasted_iota(jnp.int32, (1, NZ), 1)
        energy = jnp.sum(jnp.where(lane < NZ // 2, sums, 0.0), axis=1, keepdims=True)
        total = jnp.sum(jnp.where(lane < NZ // 2, 0.0, sums), axis=1, keepdims=True)
        total = jnp.broadcast_to(total, (1, NZ))
    else:
        energy = jnp.sum(sums, axis=1, keepdims=True)
        total = carry_ref[1:2, :]
    speed = scale * jnp.sqrt(jnp.broadcast_to(energy, (1, NZ)))
    factor = jnp.sqrt(carry_ref[HEAT_ROW + step : HEAT_ROW + step + 1, :] * total / (speed * speed + excess_coupling))
    return jnp.minimum(scale * factor, SCALE_CAP), total


def step_kernel(received_ref, carry_ref, u_in_ref, weight_ref, mass_ref, u_ref, rows_ref, out_ref, *, step, left):
    start = carry_ref[START_ROW + step : START_ROW + step + 1, :][0, 0].astype(jnp.int32)
    scale, total = next_scale(received_ref, carry_ref, step - 1)
    wide = jnp.broadcast_to(scale, (PAD, NZ))
    turn = left - (STEPS + 1 - step) // 2
    u_ref[0] = u_in_ref[0]
    u_ref[full_planes(left) - 1] = u_in_ref[full_planes(left) - 1]
    for k in range(pair_count(left)):
        plane = start + 2 * k
        low, high = u_in_ref[plane], u_in_ref[plane + 1]
        closing = jnp.maximum(low - high, 0.0)
        push = closing * jnp.tanh(wide * closing)
        u_ref[plane] = low - weight_ref[turn, 0, k] * push
        u_ref[plane + 1] = high + weight_ref[turn, 1, k] * push
    energy = jnp.zeros((PAD, NZ), f32)
    for k in range(EXT):
        u = u_ref[left + k]
        energy = energy + mass_ref[k] * u * u
    mine = fold(energy)
    other = carry_ref[4:5, :] if step % 2 == 0 else carry_ref[3:4, :]
    out_ref[...] = carry_ref[...]
    out_ref[0:1, :] = scale
    out_ref[1:2, :] = total
    row = 3 if step % 2 == 0 else 4
    out_ref[row : row + 1, :] = mine
    rows_ref[...] = jnp.broadcast_to(carry_ref[2:3, :] + mine + other, (DEVICES, NZ))


def collide(step, received, carry, u, weight, mass):
    left, _ = place_of(step)

    def body(*refs):
        step_kernel(*refs, step=step, left=left)

    return pl.pallas_call(
        body,
        in_specs=[VMEM] * 5,
        out_specs=[VMEM] * 3,
        out_shape=[shape(full_planes(left), PAD, NZ), shape(DEVICES, NZ), shape(CARRY, NZ)],
        compiler_params=GRANT,
        name="collide",
    )(received, carry, u, weight, mass)


def turn_kernel(shift_ref, v_ref, count_ref, spin_ref, w_ref):
    shifts = [later_shifts(shift_ref, step) for step in range(STEPS)]

    def plane(i, carry):
        real = jnp.ones((EXT, NZ), f32)
        parts = [jnp.zeros((EXT, NZ), f32)] * 3
        for step in range(STEPS):
            spin = pltpu.roll(spin_ref[step, i], shifts[step], 1)
            tangent = jnp.where((spin & 1) == 0, HALF_TAN, -HALF_TAN)
            on_x, on_y = spin < 2, spin < 4
            x, y, z = parts

            def pick(first, second, third):
                return tangent * jnp.where(on_x, first, jnp.where(on_y, second, third))

            real, parts = (
                real - pick(x, y, z),
                [x + pick(real, z, -y), y + pick(-z, real, x), z + pick(y, -x, real)],
            )
        x, y, z = parts
        unit = BIG * TURN_NORM
        xx, yy, zz, rr = x * x, y * y, z * z, real * real
        rows = [
            [(rr + xx) - (yy + zz), 2.0 * (x * y - real * z), 2.0 * (x * z + real * y)],
            [2.0 * (x * y + real * z), (rr + yy) - (xx + zz), 2.0 * (y * z - real * x)],
            [2.0 * (x * z - real * y), 2.0 * (y * z + real * x), (rr + zz) - (xx + yy)],
        ]
        rows = [[unit * value for value in row] for row in rows]
        counts = pltpu.roll(count_ref[i], shifts[0], 1)
        inverse = 1.0 / jnp.maximum(counts.astype(f32), 1.0)
        values = [
            [
                jnp.where(counts > slot, pltpu.roll(v_ref[member, slot, i], shifts[0], 1), 0.0)
                for slot in range(SLOTS)
            ]
            for member in range(3)
        ]
        mean = []
        for member in range(3):
            moment = values[member][0]
            for slot in range(1, SLOTS):
                moment = moment + values[member][slot]
            mean.append(moment * inverse)
        for slot in range(SLOTS):
            rest = [values[member][slot] - mean[member] for member in range(3)]
            for member in range(3):
                turned = rows[member][0] * rest[0] + rows[member][1] * rest[1] + rows[member][2] * rest[2]
                w_ref[member, slot, i] = turned
        return carry

    lax.fori_loop(0, EXT, plane, 0)


def turn(shifts, v, counts, spin):
    return pl.pallas_call(
        turn_kernel,
        in_specs=[SMEM, VMEM, VMEM, VMEM],
        out_specs=VMEM,
        out_shape=shape(3, SLOTS, EXT, EXT, NZ),
        compiler_params=GRANT,
        name="turn",
    )(shifts, v, counts, spin)


def finish_kernel(received_ref, carry_ref, ux_ref, uy_ref, uz_ref, own_ref, w_ref, v_ref):
    member = pl.program_id(0)
    scale, _ = next_scale(received_ref, carry_ref, STEPS - 1)
    wide = jnp.broadcast_to(scale, (EXT, NZ))

    def write(mean_of):
        for i in range(EXT):
            counts = own_ref[0, i, 0:EXT, :]
            mean = mean_of(i)
            for slot in range(SLOTS):
                v_ref[0, slot, i] = jnp.where(counts > slot, wide * (mean + w_ref[0, slot, i]), 0.0)

    @pl.when(member == 0)
    def _():
        write(lambda i: ux_ref[X_LEFT + i, 0:EXT, :])

    @pl.when(member == 1)
    def _():
        write(lambda i: uy_ref[pl.ds(Y_LEFT * PAD + i, EXT, stride=PAD), :])

    @pl.when(member == 2)
    def _():
        write(lambda i: uz_ref[i, 0:EXT, :])


def finish(received, carry, ux, uy, uz, own, w):
    part = pl.BlockSpec((1, SLOTS, EXT, EXT, NZ), lambda c: (c, 0, 0, 0, 0))
    mass = pl.BlockSpec((1, EXT, PAD, NZ), lambda c: (1, 0, 0, 0))
    return pl.pallas_call(
        finish_kernel,
        grid=(3,),
        in_specs=[VMEM] * 5 + [mass, part],
        out_specs=part,
        out_shape=shape(3, SLOTS, EXT, EXT, NZ),
        compiler_params=GRANT,
        name="finish",
    )(received, carry, ux, uy.reshape(full_planes(Y_LEFT) * PAD, NZ), uz, own, w)


def exchange(low_edge, high_edge, axis):
    count = lax.axis_size(axis)
    down = [(source, (source - 1) % count) for source in range(count)]
    up = [(source, (source + 1) % count) for source in range(count)]
    return lax.ppermute(low_edge, axis, down), lax.ppermute(high_edge, axis, up)


def sum_over_devices(rows):
    return lax.all_to_all(rows, ("bx", "by"), 0, 0, tiled=True)


def per_device(v, counts, spin, flags, parity, shifts, heat):
    own, uy, uz, low, high, carry = prep(shifts, parity, heat, v, counts, flags)
    above, below = exchange(low, high, "bx")
    bits, sy, ylo, yhi = spread(shifts, own, uy, flags)
    y_above, y_below = exchange(ylo, yhi, "by")
    rows, carry, sx, xlo, xhi = first(parity, own, bits, below, above, carry)
    received = sum_over_devices(rows)
    x_above, x_below = exchange(xlo, xhi, "bx")
    uy, y_weights, y_mass = join(parity, sy, y_below, y_above, Y_LEFT, "by")
    ux, x_weights, x_mass = join(parity, sx, x_below, x_above, X_LEFT, "bx")
    for step in range(1, STEPS):
        if step % 2 == 0:
            ux, rows, carry = collide(step, received, carry, ux, x_weights, x_mass)
        else:
            uy, rows, carry = collide(step, received, carry, uy, y_weights, y_mass)
        received = sum_over_devices(rows)
        if step == TURN_STEP:
            received, shifts = lax.optimization_barrier((received, shifts))
            w = turn(shifts, v, counts, spin)
            received, w = lax.optimization_barrier((received, w))
    return finish(received, carry, ux, uy, uz, own, w)


def solution(mesh):
    return jax.shard_map(
        per_device,
        mesh=mesh,
        in_specs=(
            P(None, None, "bx", "by", None),
            P("bx", "by", None),
            P(None, "bx", "by", None),
            P(None, "bx", "by", None),
            P(),
            P(),
            P(),
        ),
        out_specs=P(None, None, "bx", "by", None),
        check_vma=False,
    )
```

```python
import math

import jax
import jax.numpy as jnp
from jax import lax
from jax.experimental import pallas as pl
from jax.experimental.pallas import tpu as pltpu
from jax.sharding import PartitionSpec as P

STEPS = 12
HALF = STEPS // 2
SLOTS = 6
EXT = 15
PAD = 16
CHUNK = 3
TURN_STEP = 5
NZ = 128
DEVICES = 128
X_LEFT = HALF - 1
Y_LEFT = HALF
HEAT_ROW = 8
START_ROW = HEAT_ROW + PAD
SHIFT_ROW = START_ROW + PAD
CARRY = SHIFT_ROW + PAD

turn_angle = 130.0 * math.pi / 180.0
excess_coupling = 1e-06
BIG = 2.0**46
SCALE_CAP = 3e38
HALF_TAN = math.tan(turn_angle / 2.0)
TURN_NORM = math.cos(turn_angle / 2.0) ** (2 * STEPS)

VMEM = pl.BlockSpec(memory_space=pltpu.VMEM)
SMEM = pl.BlockSpec(memory_space=pltpu.SMEM)
ANY = pl.BlockSpec(memory_space=pl.ANY)
f32 = jnp.float32
GRANT = pltpu.CompilerParams(vmem_limit_bytes=12 * 2**20)


def shape(*dims):
    return jax.ShapeDtypeStruct(dims, f32)


def later_shifts(shift_ref, step):
    total = jnp.int32(0)
    for later in range(step, STEPS):
        total = total + shift_ref[later]
    return lax.rem(total, jnp.int32(NZ))


def edge_layout(left):
    counts = [left, left] + [left - k for k in range(left)]
    starts = [sum(counts[:k]) for k in range(len(counts))]
    return list(zip(starts, counts)), sum(counts)


def full_planes(left):
    return EXT + 2 * left


def pair_count(left):
    return (full_planes(left) - 1) // 2


def whole(carry_ref, row):
    return carry_ref[row : row + 1, :][0, 0].astype(jnp.int32)


def place_of(step):
    return (X_LEFT, "bx") if step % 2 == 0 else (Y_LEFT, "by")


def fold(values):
    return jnp.sum(values, axis=0, keepdims=True)


def prep_kernel(
    shift_hbm, parity_hbm, heat_hbm, v_hbm, count_hbm, flag_hbm,
    ux_ref, mass_ref, allow_ref, uy_ref, uz_ref, low_ref, high_ref, base_ref,
    shift_ref, parity_ref, heat_ref, v_ref, count_ref, flag_ref, sems, chunk_sems,
):
    fetches = [
        pltpu.make_async_copy(shift_hbm, shift_ref, sems.at[0]),
        pltpu.make_async_copy(count_hbm, count_ref, sems.at[1]),
        pltpu.make_async_copy(flag_hbm.at[0], flag_ref, sems.at[2]),
        pltpu.make_async_copy(parity_hbm, parity_ref, sems.at[3]),
        pltpu.make_async_copy(heat_hbm, heat_ref, sems.at[4]),
    ]
    chunks = [
        pltpu.make_async_copy(
            v_hbm.at[:, :, pl.ds(CHUNK * c, CHUNK)], v_ref.at[:, :, pl.ds(CHUNK * c, CHUNK)], chunk_sems.at[c]
        )
        for c in range(EXT // CHUNK)
    ]
    for fetch in fetches + chunks:
        fetch.start()
    for fetch in fetches:
        fetch.wait()
    shift = later_shifts(shift_ref, 0)
    zero_row = jnp.zeros((EXT, 1, NZ), f32)
    for array_ref in (ux_ref, mass_ref, allow_ref, uy_ref, uz_ref):
        array_ref[0:EXT, EXT:PAD, :] = zero_row
    uy_ref[EXT] = jnp.zeros((PAD, NZ), f32)

    thermal = energy_y = total = jnp.zeros((EXT, NZ), f32)
    for i in range(EXT):
        if i % CHUNK == 0:
            chunks[i // CHUNK].wait()
        counts = count_ref[i]
        mass = counts.astype(f32)
        inverse = 1.0 / jnp.maximum(mass, 1.0)
        mean = []
        for member in range(3):
            values = [
                jnp.where(counts > slot, v_ref[member, slot, i] * BIG, 0.0) for slot in range(SLOTS)
            ]
            moment = values[0]
            for slot in range(1, SLOTS):
                moment = moment + values[slot]
            middle = moment * inverse
            mean.append(middle)
            for slot in range(SLOTS):
                rest = jnp.where(counts > slot, values[slot] - middle, 0.0)
                thermal = thermal + rest * rest
        thermal = thermal + mass * mean[2] * mean[2]
        energy_y = energy_y + mass * mean[1] * mean[1]
        total = total + mass
        ux_ref[i, 0:EXT, :] = pltpu.roll(mean[0], shift, 1)
        mass_ref[i, 0:EXT, :] = pltpu.roll(mass, shift, 1)
        allow_ref[i, 0:EXT, :] = pltpu.roll(flag_ref[i].astype(f32), shift, 1)
        uy_ref[i, 0:EXT, :] = pltpu.roll(mean[1], shift, 1)
        uz_ref[i, 0:EXT, :] = pltpu.roll(mean[2], shift, 1)
    base_ref[...] = jnp.zeros((CARRY, NZ), f32)
    for step in range(STEPS):
        left, brick_axis = place_of(step)
        start = lower_start(parity_ref, step, brick_axis, left)
        base_ref[HEAT_ROW + step : HEAT_ROW + step + 1, :] = jnp.full((1, NZ), 3.0 * heat_ref[step], f32)
        base_ref[START_ROW + step : START_ROW + step + 1, :] = jnp.full((1, NZ), start.astype(f32), f32)
        later = later_shifts(shift_ref, step)
        base_ref[SHIFT_ROW + step : SHIFT_ROW + step + 1, :] = jnp.full((1, NZ), later.astype(f32), f32)
    base_ref[0:1, :] = jnp.full((1, NZ), 1.0 / BIG, f32)
    base_ref[2:3, :] = fold(thermal)
    base_ref[4:5, :] = fold(energy_y)
    base_ref[5:6, :] = fold(total)
    for field, array_ref in enumerate((ux_ref, mass_ref, allow_ref)):
        low_ref[field] = array_ref[0]
        high_ref[field] = array_ref[EXT - 1]


def prep(shifts, parity, heat, v, counts, flags):
    edge = shape(3, PAD, NZ)
    return pl.pallas_call(
        prep_kernel,
        in_specs=[ANY] * 6,
        out_specs=[VMEM] * 8,
        out_shape=[shape(EXT, PAD, NZ)] * 3 + [shape(PAD, PAD, NZ), shape(EXT, PAD, NZ), edge, edge, shape(CARRY, NZ)],
        scratch_shapes=[
            pltpu.SMEM((STEPS,), jnp.int32),
            pltpu.SMEM((STEPS,), jnp.int32),
            pltpu.SMEM((STEPS,), f32),
            pltpu.VMEM((3, SLOTS, EXT, EXT, NZ), f32),
            pltpu.VMEM((EXT, EXT, NZ), jnp.int32),
            pltpu.VMEM((EXT, EXT, NZ), jnp.int32),
            pltpu.SemaphoreType.DMA((5,)),
            pltpu.SemaphoreType.DMA((EXT // CHUNK,)),
        ],
        compiler_params=GRANT,
        name="prep",
    )(*[pltpu.with_memory_space_constraint(array, pltpu.HBM) for array in (shifts, parity, heat, v, counts, flags)])


def spread_kernel(carry_ref, mass_ref, uy_ref, flag_ref, bits_ref, own_ref, y_mass_ref, y_bits_ref, low_ref, high_ref, turn_ref):
    bits_ref[:, :, EXT:PAD, :] = jnp.zeros((X_LEFT, EXT, 1, NZ), f32)
    for step in range(1, STEPS):
        later = whole(carry_ref, SHIFT_ROW + step)
        for i in range(EXT):
            bits = pltpu.roll(flag_ref[step, i].astype(f32), later, 1)
            if step % 2 == 0:
                bits_ref[step // 2 - 1, i, 0:EXT, :] = bits
            else:
                turn_ref[step // 2, i * PAD : i * PAD + EXT, :] = bits
    keep = lax.broadcasted_iota(jnp.int32, (PAD, NZ), 0) < EXT
    for i in range(EXT):
        turn_ref[HALF, i * PAD : (i + 1) * PAD, :] = mass_ref[i]
    for field, (place, planes) in enumerate(edge_layout(Y_LEFT)[0]):
        for y in range(EXT):
            line = pl.ds(y, PAD, stride=PAD)
            if field == 0:
                rows = own_ref[y] = jnp.where(keep, uy_ref[line, :], 0.0)
            elif field == 1:
                rows = y_mass_ref[y] = jnp.where(keep, turn_ref[HALF, line, :], 0.0)
            else:
                rows = y_bits_ref[field - 2, y] = jnp.where(keep, turn_ref[field - 2, line, :], 0.0)
            if y < planes:
                low_ref[place + y] = rows
            if y >= EXT - planes:
                high_ref[place + y - (EXT - planes)] = rows


def spread(carry, mass, uy, flags):
    edge = shape(edge_layout(Y_LEFT)[1], PAD, NZ)
    plane = shape(EXT, PAD, NZ)
    return pl.pallas_call(
        spread_kernel,
        in_specs=[VMEM] * 4,
        out_specs=[VMEM] * 6,
        out_shape=[shape(X_LEFT, EXT, PAD, NZ), plane, plane, shape(Y_LEFT, EXT, PAD, NZ), edge, edge],
        scratch_shapes=[pltpu.VMEM((HALF + 1, PAD * PAD, NZ), f32)],
        compiler_params=GRANT,
        name="spread",
    )(carry, mass, uy.reshape(PAD * PAD, NZ), flags)


def lower_start(parity_ref, step, brick_axis, halo):
    return lax.rem(parity_ref[step] + lax.axis_index(brick_axis) * EXT + halo, jnp.int32(2))


def first_kernel(
    carry_ref, own_ref, own_mass_ref, own_allow_ref, bits_ref, below_ref, above_ref,
    rows_ref, out_ref, next_ref, xlo_ref, xhi_ref, u_ref, mass_ref, allow_ref,
):
    for field, (all_ref, mine_ref) in enumerate(
        ((u_ref, own_ref), (mass_ref, own_mass_ref), (allow_ref, own_allow_ref))
    ):
        all_ref[0] = below_ref[field]
        all_ref[EXT + 1] = above_ref[field]
        for k in range(EXT):
            all_ref[1 + k] = mine_ref[k]
    start = whole(carry_ref, START_ROW)
    wide = jnp.broadcast_to(carry_ref[0:1, :], (PAD, NZ))
    for k in range((EXT + 1) // 2):
        plane = start + 2 * k
        low, high = u_ref[plane], u_ref[plane + 1]
        weight_low, weight_high = pair_weights(mass_ref[plane], mass_ref[plane + 1])
        allowed = jnp.maximum(allow_ref[plane], allow_ref[plane + 1])
        closing = jnp.maximum(low - high, 0.0)
        push = allowed * closing * jnp.tanh(wide * closing)
        u_ref[plane] = low - weight_low * push
        u_ref[plane + 1] = high + weight_high * push
    energy = jnp.zeros((PAD, NZ), f32)
    for k in range(EXT):
        u = u_ref[1 + k]
        energy = energy + own_mass_ref[k] * u * u
        next_ref[k] = u
    for field, (place, planes) in enumerate(edge_layout(X_LEFT)[0]):
        for k in range(planes):
            for edge_ref, plane in ((xlo_ref, k), (xhi_ref, EXT - planes + k)):
                if field == 0:
                    edge_ref[place + k] = next_ref[plane]
                elif field == 1:
                    edge_ref[place + k] = own_mass_ref[plane]
                else:
                    edge_ref[place + k] = bits_ref[field - 2, plane]
    mine = fold(energy)
    half = NZ // 2
    lane = lax.broadcasted_iota(jnp.int32, (1, NZ), 1)
    local = carry_ref[2:3, :] + mine + carry_ref[4:5, :]
    number = carry_ref[5:6, :]
    local = jnp.where(lane < half, local + pltpu.roll(local, half, 1), number + pltpu.roll(number, half, 1))
    out_ref[...] = carry_ref[...]
    out_ref[3:4, :] = mine
    rows_ref[...] = jnp.broadcast_to(local, (DEVICES, NZ))


def first(carry, own, mass, allow, bits, below, above):
    edge = shape(edge_layout(X_LEFT)[1], PAD, NZ)
    return pl.pallas_call(
        first_kernel,
        in_specs=[VMEM] * 7,
        out_specs=[VMEM] * 5,
        out_shape=[shape(DEVICES, NZ), shape(CARRY, NZ), shape(EXT, PAD, NZ), edge, edge],
        scratch_shapes=[pltpu.VMEM((EXT + 2, PAD, NZ), f32)] * 3,
        compiler_params=GRANT,
        name="first",
    )(carry, own, mass, allow, bits, below, above)


def pair_weights(mass_low, mass_high):
    reduced = mass_low * mass_high / jnp.maximum(mass_low + mass_high, 1.0)
    return reduced / jnp.maximum(mass_low, 1.0), reduced / jnp.maximum(mass_high, 1.0)


def join_kernel(
    carry_ref, own_ref, mass_ref, own_bits_ref, below_ref, above_ref, u_ref, weight_ref, all_mass_ref, bits_ref, both_ref, *, left, first_step
):
    for field, (place, planes) in enumerate(edge_layout(left)[0]):
        for k in range(planes):
            low, high = below_ref[place + k], above_ref[place + k]
            below, above = left - planes + k, left + EXT + k
            if field == 0:
                u_ref[below], u_ref[above] = low, high
            elif field == 1:
                all_mass_ref[below], all_mass_ref[above] = low, high
            else:
                bits_ref[field - 2, below], bits_ref[field - 2, above] = low, high
        for k in range(left - planes):
            bits_ref[field - 2, k] = jnp.zeros((PAD, NZ), f32)
            bits_ref[field - 2, full_planes(left) - 1 - k] = jnp.zeros((PAD, NZ), f32)
    for k in range(EXT):
        u_ref[left + k] = own_ref[k]
        all_mass_ref[left + k] = mass_ref[k]
        for j in range(left):
            bits_ref[j, left + k] = own_bits_ref[j, k]
    for plane in range(full_planes(left) - 1):
        both_ref[0, plane], both_ref[1, plane] = pair_weights(all_mass_ref[plane], all_mass_ref[plane + 1])
    for j in range(left):
        start = whole(carry_ref, START_ROW + first_step + 2 * j)
        for k in range(pair_count(left)):
            plane = start + 2 * k
            allowed = jnp.maximum(bits_ref[j, plane], bits_ref[j, plane + 1])
            weight_ref[j, 0, k] = allowed * both_ref[0, plane]
            weight_ref[j, 1, k] = allowed * both_ref[1, plane]


def join(carry, own, mass, bits, below, above, left, first_step):
    def body(*refs):
        join_kernel(*refs, left=left, first_step=first_step)

    full, pairs = full_planes(left), pair_count(left)
    return pl.pallas_call(
        body,
        in_specs=[VMEM] * 6,
        out_specs=[VMEM] * 2,
        out_shape=[shape(full, PAD, NZ), shape(left, 2, pairs, PAD, NZ)],
        scratch_shapes=[
            pltpu.VMEM((full, PAD, NZ), f32),
            pltpu.VMEM((left, full, PAD, NZ), f32),
            pltpu.VMEM((2, full, PAD, NZ), f32),
        ],
        compiler_params=GRANT,
        name="join",
    )(carry, own, mass, bits, below, above)


def next_scale(received_ref, carry_ref, step):
    sums = jnp.sum(received_ref[...], axis=0, keepdims=True)
    scale = carry_ref[0:1, :]
    if step == 0:
        lane = lax.broadcasted_iota(jnp.int32, (1, NZ), 1)
        energy = jnp.sum(jnp.where(lane < NZ // 2, sums, 0.0), axis=1, keepdims=True)
        total = jnp.sum(jnp.where(lane < NZ // 2, 0.0, sums), axis=1, keepdims=True)
        total = jnp.broadcast_to(total, (1, NZ))
    else:
        energy = jnp.sum(sums, axis=1, keepdims=True)
        total = carry_ref[1:2, :]
    speed = scale * jnp.sqrt(jnp.broadcast_to(energy, (1, NZ)))
    factor = jnp.sqrt(carry_ref[HEAT_ROW + step : HEAT_ROW + step + 1, :] * total / (speed * speed + excess_coupling))
    return jnp.minimum(scale * factor, SCALE_CAP), total


def step_kernel(received_ref, carry_ref, u_in_ref, weight_ref, mass_ref, u_ref, rows_ref, out_ref, *, step, left):
    start = whole(carry_ref, START_ROW + step)
    scale, total = next_scale(received_ref, carry_ref, step - 1)
    wide = jnp.broadcast_to(scale, (PAD, NZ))
    turn = left - (STEPS + 1 - step) // 2
    u_ref[0] = u_in_ref[0]
    u_ref[full_planes(left) - 1] = u_in_ref[full_planes(left) - 1]
    for k in range(pair_count(left)):
        plane = start + 2 * k
        low, high = u_in_ref[plane], u_in_ref[plane + 1]
        closing = jnp.maximum(low - high, 0.0)
        push = closing * jnp.tanh(wide * closing)
        u_ref[plane] = low - weight_ref[turn, 0, k] * push
        u_ref[plane + 1] = high + weight_ref[turn, 1, k] * push
    energy = jnp.zeros((PAD, NZ), f32)
    for k in range(EXT):
        u = u_ref[left + k]
        energy = energy + mass_ref[k] * u * u
    mine = fold(energy)
    other = carry_ref[4:5, :] if step % 2 == 0 else carry_ref[3:4, :]
    out_ref[...] = carry_ref[...]
    out_ref[0:1, :] = scale
    out_ref[1:2, :] = total
    row = 3 if step % 2 == 0 else 4
    out_ref[row : row + 1, :] = mine
    rows_ref[...] = jnp.broadcast_to(carry_ref[2:3, :] + mine + other, (DEVICES, NZ))


def collide(step, received, carry, u, weight, mass):
    left, _ = place_of(step)

    def body(*refs):
        step_kernel(*refs, step=step, left=left)

    return pl.pallas_call(
        body,
        in_specs=[VMEM] * 5,
        out_specs=[VMEM] * 3,
        out_shape=[shape(full_planes(left), PAD, NZ), shape(DEVICES, NZ), shape(CARRY, NZ)],
        compiler_params=GRANT,
        name="collide",
    )(received, carry, u, weight, mass)


def turn_kernel(carry_ref, v_ref, count_ref, spin_ref, w_ref):
    shifts = [whole(carry_ref, SHIFT_ROW + step) for step in range(STEPS)]

    def plane(i, carry):
        real = jnp.ones((EXT, NZ), f32)
        parts = [jnp.zeros((EXT, NZ), f32)] * 3
        for step in range(STEPS):
            spin = pltpu.roll(spin_ref[step, i], shifts[step], 1)
            tangent = jnp.where((spin & 1) == 0, HALF_TAN, -HALF_TAN)
            on_x, on_y = spin < 2, spin < 4
            x, y, z = parts

            def pick(first, second, third):
                return tangent * jnp.where(on_x, first, jnp.where(on_y, second, third))

            real, parts = (
                real - pick(x, y, z),
                [x + pick(real, z, -y), y + pick(-z, real, x), z + pick(y, -x, real)],
            )
        x, y, z = parts
        unit = BIG * TURN_NORM
        xx, yy, zz, rr = x * x, y * y, z * z, real * real
        rows = [
            [(rr + xx) - (yy + zz), 2.0 * (x * y - real * z), 2.0 * (x * z + real * y)],
            [2.0 * (x * y + real * z), (rr + yy) - (xx + zz), 2.0 * (y * z - real * x)],
            [2.0 * (x * z - real * y), 2.0 * (y * z + real * x), (rr + zz) - (xx + yy)],
        ]
        rows = [[unit * value for value in row] for row in rows]
        counts = pltpu.roll(count_ref[i], shifts[0], 1)
        inverse = 1.0 / jnp.maximum(counts.astype(f32), 1.0)
        values = [
            [
                jnp.where(counts > slot, pltpu.roll(v_ref[member, slot, i], shifts[0], 1), 0.0)
                for slot in range(SLOTS)
            ]
            for member in range(3)
        ]
        mean = []
        for member in range(3):
            moment = values[member][0]
            for slot in range(1, SLOTS):
                moment = moment + values[member][slot]
            mean.append(moment * inverse)
        for slot in range(SLOTS):
            rest = [values[member][slot] - mean[member] for member in range(3)]
            for member in range(3):
                turned = rows[member][0] * rest[0] + rows[member][1] * rest[1] + rows[member][2] * rest[2]
                w_ref[member, slot, i] = turned
        return carry

    lax.fori_loop(0, EXT, plane, 0)


def turn(carry, v, counts, spin):
    return pl.pallas_call(
        turn_kernel,
        in_specs=[VMEM] * 4,
        out_specs=VMEM,
        out_shape=shape(3, SLOTS, EXT, EXT, NZ),
        compiler_params=GRANT,
        name="turn",
    )(carry, v, counts, spin)


def finish_kernel(received_ref, carry_ref, ux_ref, uy_ref, uz_ref, mass_ref, w_ref, v_ref):
    member = pl.program_id(0)
    scale, _ = next_scale(received_ref, carry_ref, STEPS - 1)
    wide = jnp.broadcast_to(scale, (EXT, NZ))

    def write(mean_of):
        for i in range(EXT):
            counts = mass_ref[i, 0:EXT, :]
            mean = mean_of(i)
            for slot in range(SLOTS):
                v_ref[0, slot, i] = jnp.where(counts > slot, wide * (mean + w_ref[0, slot, i]), 0.0)

    @pl.when(member == 0)
    def _():
        write(lambda i: ux_ref[X_LEFT + i, 0:EXT, :])

    @pl.when(member == 1)
    def _():
        write(lambda i: uy_ref[pl.ds(Y_LEFT * PAD + i, EXT, stride=PAD), :])

    @pl.when(member == 2)
    def _():
        write(lambda i: uz_ref[i, 0:EXT, :])


def finish(received, carry, ux, uy, uz, mass, w):
    part = pl.BlockSpec((1, SLOTS, EXT, EXT, NZ), lambda c: (c, 0, 0, 0, 0))
    return pl.pallas_call(
        finish_kernel,
        grid=(3,),
        in_specs=[VMEM] * 6 + [part],
        out_specs=part,
        out_shape=shape(3, SLOTS, EXT, EXT, NZ),
        compiler_params=GRANT,
        name="finish",
    )(received, carry, ux, uy.reshape(full_planes(Y_LEFT) * PAD, NZ), uz, mass, w)


def exchange(low_edge, high_edge, axis):
    count = lax.axis_size(axis)
    down = [(source, (source - 1) % count) for source in range(count)]
    up = [(source, (source + 1) % count) for source in range(count)]
    return lax.ppermute(low_edge, axis, down), lax.ppermute(high_edge, axis, up)


def sum_over_devices(rows):
    return lax.all_to_all(rows, ("bx", "by"), 0, 0, tiled=True)


def per_device(v, counts, spin, flags, parity, shifts, heat):
    ux, mass, allow, uy, uz, low, high, carry = prep(shifts, parity, heat, v, counts, flags)
    above, below = exchange(low, high, "bx")
    bits, uy, y_mass, y_bits, ylo, yhi = spread(carry, mass, uy, flags)
    y_above, y_below = exchange(ylo, yhi, "by")
    rows, carry, ux, xlo, xhi = first(carry, ux, mass, allow, bits, below, above)
    received = sum_over_devices(rows)
    x_above, x_below = exchange(xlo, xhi, "bx")
    received, carry, uy = lax.optimization_barrier((received, carry, uy))
    uy, y_weights = join(carry, uy, y_mass, y_bits, y_below, y_above, Y_LEFT, 1)
    for step in range(1, STEPS):
        if step % 2 == 0:
            ux, rows, carry = collide(step, received, carry, ux, x_weights, mass)
        else:
            uy, rows, carry = collide(step, received, carry, uy, y_weights, y_mass)
        received = sum_over_devices(rows)
        if step == 1:
            received, carry, ux = lax.optimization_barrier((received, carry, ux))
            ux, x_weights = join(carry, ux, mass, bits, x_below, x_above, X_LEFT, 2)
        if step == TURN_STEP:
            received, carry = lax.optimization_barrier((received, carry))
            w = turn(carry, v, counts, spin)
            received, w = lax.optimization_barrier((received, w))
    return finish(received, carry, ux, uy, uz, mass, w)


def solution(mesh):
    return jax.shard_map(
        per_device,
        mesh=mesh,
        in_specs=(
            P(None, None, "bx", "by", None),
            P("bx", "by", None),
            P(None, "bx", "by", None),
            P(None, "bx", "by", None),
            P(),
            P(),
            P(),
        ),
        out_specs=P(None, None, "bx", "by", None),
        check_vma=False,
    )
```

```python
import math

import jax
import jax.numpy as jnp
from jax import lax
from jax.experimental import pallas as pl
from jax.experimental.pallas import tpu as pltpu
from jax.sharding import PartitionSpec as P

STEPS = 12
HALF = STEPS // 2
SLOTS = 6
EXT = 15
PAD = 16
CHUNK = 3
NZ = 128
DEVICES = 128
X_LEFT = HALF - 1
Y_LEFT = HALF
HEAT_ROW = 8
START_ROW = HEAT_ROW + PAD
SHIFT_ROW = START_ROW + PAD
CARRY = SHIFT_ROW + PAD

turn_angle = 130.0 * math.pi / 180.0
excess_coupling = 1e-06
BIG = 2.0**46
SCALE_CAP = 3e38
HALF_TAN = math.tan(turn_angle / 2.0)
TURN_NORM = math.cos(turn_angle / 2.0) ** (2 * STEPS)

VMEM = pl.BlockSpec(memory_space=pltpu.VMEM)
SMEM = pl.BlockSpec(memory_space=pltpu.SMEM)
ANY = pl.BlockSpec(memory_space=pl.ANY)
f32 = jnp.float32
GRANT = pltpu.CompilerParams(vmem_limit_bytes=12 * 2**20)


def shape(*dims):
    return jax.ShapeDtypeStruct(dims, f32)


def far(*dims):
    return pltpu.HBM(dims, f32)


def later_shifts(shift_ref, step):
    total = jnp.int32(0)
    for later in range(step, STEPS):
        total = total + shift_ref[later]
    return lax.rem(total, jnp.int32(NZ))


def edge_layout(left):
    counts = [left, left] + [left - k for k in range(left)]
    starts = [sum(counts[:k]) for k in range(len(counts))]
    return list(zip(starts, counts)), sum(counts)


def full_planes(left):
    return EXT + 2 * left


def pair_count(left):
    return (full_planes(left) - 1) // 2


def whole(carry_ref, row):
    return carry_ref[row : row + 1, :][0, 0].astype(jnp.int32)


def place_of(step):
    return (X_LEFT, "bx") if step % 2 == 0 else (Y_LEFT, "by")


def fold(values):
    return jnp.sum(values, axis=0, keepdims=True)


def prep_kernel(
    shift_hbm, parity_hbm, heat_hbm, v_hbm, count_hbm, flag_hbm,
    ux_ref, mass_ref, allow_ref, uy_ref, uz_ref, low_ref, high_ref, base_ref,
    shift_ref, parity_ref, heat_ref, v_ref, count_ref, flag_ref, sems, chunk_sems,
):
    fetches = [
        pltpu.make_async_copy(shift_hbm, shift_ref, sems.at[0]),
        pltpu.make_async_copy(count_hbm, count_ref, sems.at[1]),
        pltpu.make_async_copy(flag_hbm.at[0], flag_ref, sems.at[2]),
        pltpu.make_async_copy(parity_hbm, parity_ref, sems.at[3]),
        pltpu.make_async_copy(heat_hbm, heat_ref, sems.at[4]),
    ]
    chunks = [
        pltpu.make_async_copy(
            v_hbm.at[:, :, pl.ds(CHUNK * c, CHUNK)], v_ref.at[:, :, pl.ds(CHUNK * c, CHUNK)], chunk_sems.at[c]
        )
        for c in range(EXT // CHUNK)
    ]
    for fetch in fetches + chunks:
        fetch.start()
    for fetch in fetches:
        fetch.wait()
    shift = later_shifts(shift_ref, 0)
    zero_row = jnp.zeros((EXT, 1, NZ), f32)
    for array_ref in (ux_ref, mass_ref, allow_ref, uy_ref, uz_ref):
        array_ref[0:EXT, EXT:PAD, :] = zero_row
    uy_ref[EXT] = jnp.zeros((PAD, NZ), f32)

    thermal = energy_y = total = jnp.zeros((EXT, NZ), f32)
    for i in range(EXT):
        if i % CHUNK == 0:
            chunks[i // CHUNK].wait()
        counts = count_ref[i]
        mass = counts.astype(f32)
        inverse = 1.0 / jnp.maximum(mass, 1.0)
        mean = []
        for member in range(3):
            values = [
                jnp.where(counts > slot, v_ref[member, slot, i] * BIG, 0.0) for slot in range(SLOTS)
            ]
            moment = values[0]
            for slot in range(1, SLOTS):
                moment = moment + values[slot]
            middle = moment * inverse
            mean.append(middle)
            for slot in range(SLOTS):
                rest = jnp.where(counts > slot, values[slot] - middle, 0.0)
                thermal = thermal + rest * rest
        thermal = thermal + mass * mean[2] * mean[2]
        energy_y = energy_y + mass * mean[1] * mean[1]
        total = total + mass
        ux_ref[i, 0:EXT, :] = pltpu.roll(mean[0], shift, 1)
        mass_ref[i, 0:EXT, :] = pltpu.roll(mass, shift, 1)
        allow_ref[i, 0:EXT, :] = pltpu.roll(flag_ref[i].astype(f32), shift, 1)
        uy_ref[i, 0:EXT, :] = pltpu.roll(mean[1], shift, 1)
        uz_ref[i, 0:EXT, :] = pltpu.roll(mean[2], shift, 1)
    base_ref[...] = jnp.zeros((CARRY, NZ), f32)
    for step in range(STEPS):
        left, brick_axis = place_of(step)
        start = lower_start(parity_ref, step, brick_axis, left)
        base_ref[HEAT_ROW + step : HEAT_ROW + step + 1, :] = jnp.full((1, NZ), 3.0 * heat_ref[step], f32)
        base_ref[START_ROW + step : START_ROW + step + 1, :] = jnp.full((1, NZ), start.astype(f32), f32)
        later = later_shifts(shift_ref, step)
        base_ref[SHIFT_ROW + step : SHIFT_ROW + step + 1, :] = jnp.full((1, NZ), later.astype(f32), f32)
    base_ref[0:1, :] = jnp.full((1, NZ), 1.0 / BIG, f32)
    base_ref[2:3, :] = fold(thermal)
    base_ref[4:5, :] = fold(energy_y)
    base_ref[5:6, :] = fold(total)
    for field, array_ref in enumerate((ux_ref, mass_ref, allow_ref)):
        low_ref[field] = array_ref[0]
        high_ref[field] = array_ref[EXT - 1]


def prep(shifts, parity, heat, v, counts, flags):
    edge = shape(3, PAD, NZ)
    return pl.pallas_call(
        prep_kernel,
        in_specs=[ANY] * 6,
        out_specs=[VMEM] * 8,
        out_shape=[shape(EXT, PAD, NZ)] * 3 + [shape(PAD, PAD, NZ), shape(EXT, PAD, NZ), edge, edge, shape(CARRY, NZ)],
        scratch_shapes=[
            pltpu.SMEM((STEPS,), jnp.int32),
            pltpu.SMEM((STEPS,), jnp.int32),
            pltpu.SMEM((STEPS,), f32),
            pltpu.VMEM((3, SLOTS, EXT, EXT, NZ), f32),
            pltpu.VMEM((EXT, EXT, NZ), jnp.int32),
            pltpu.VMEM((EXT, EXT, NZ), jnp.int32),
            pltpu.SemaphoreType.DMA((5,)),
            pltpu.SemaphoreType.DMA((EXT // CHUNK,)),
        ],
        compiler_params=GRANT,
        name="prep",
    )(*[pltpu.with_memory_space_constraint(array, pltpu.HBM) for array in (shifts, parity, heat, v, counts, flags)])


def spread_kernel(carry_ref, mass_ref, uy_ref, flag_ref, bits_ref, own_ref, y_mass_ref, y_bits_ref, low_ref, high_ref, turn_ref):
    bits_ref[:, :, EXT:PAD, :] = jnp.zeros((X_LEFT, EXT, 1, NZ), f32)
    for step in range(1, STEPS):
        later = whole(carry_ref, SHIFT_ROW + step)
        for i in range(EXT):
            bits = pltpu.roll(flag_ref[step, i].astype(f32), later, 1)
            if step % 2 == 0:
                bits_ref[step // 2 - 1, i, 0:EXT, :] = bits
            else:
                turn_ref[step // 2, i * PAD : i * PAD + EXT, :] = bits
    keep = lax.broadcasted_iota(jnp.int32, (PAD, NZ), 0) < EXT
    for i in range(EXT):
        turn_ref[HALF, i * PAD : (i + 1) * PAD, :] = mass_ref[i]
    for field, (place, planes) in enumerate(edge_layout(Y_LEFT)[0]):
        for y in range(EXT):
            line = pl.ds(y, PAD, stride=PAD)
            if field == 0:
                rows = own_ref[y] = jnp.where(keep, uy_ref[line, :], 0.0)
            elif field == 1:
                rows = y_mass_ref[y] = jnp.where(keep, turn_ref[HALF, line, :], 0.0)
            else:
                rows = y_bits_ref[field - 2, y] = jnp.where(keep, turn_ref[field - 2, line, :], 0.0)
            if y < planes:
                low_ref[place + y] = rows
            if y >= EXT - planes:
                high_ref[place + y - (EXT - planes)] = rows


def spread(carry, mass, uy, flags):
    edge = shape(edge_layout(Y_LEFT)[1], PAD, NZ)
    plane = shape(EXT, PAD, NZ)
    return pl.pallas_call(
        spread_kernel,
        in_specs=[VMEM] * 4,
        out_specs=[VMEM] * 6,
        out_shape=[shape(X_LEFT, EXT, PAD, NZ), plane, plane, shape(Y_LEFT, EXT, PAD, NZ), edge, edge],
        scratch_shapes=[pltpu.VMEM((HALF + 1, PAD * PAD, NZ), f32)],
        compiler_params=GRANT,
        name="spread",
    )(carry, mass, uy.reshape(PAD * PAD, NZ), flags)


def lower_start(parity_ref, step, brick_axis, halo):
    return lax.rem(parity_ref[step] + lax.axis_index(brick_axis) * EXT + halo, jnp.int32(2))


def first_kernel(
    carry_ref, own_ref, own_mass_ref, own_allow_ref, bits_ref, below_ref, above_ref,
    rows_ref, out_ref, next_ref, xlo_hbm, xhi_hbm, u_ref, mass_ref, allow_ref, xlo_ref, xhi_ref, sems,
):
    for field, (all_ref, mine_ref) in enumerate(
        ((u_ref, own_ref), (mass_ref, own_mass_ref), (allow_ref, own_allow_ref))
    ):
        all_ref[0] = below_ref[field]
        all_ref[EXT + 1] = above_ref[field]
        for k in range(EXT):
            all_ref[1 + k] = mine_ref[k]
    start = whole(carry_ref, START_ROW)
    wide = jnp.broadcast_to(carry_ref[0:1, :], (PAD, NZ))
    for k in range((EXT + 1) // 2):
        plane = start + 2 * k
        low, high = u_ref[plane], u_ref[plane + 1]
        weight_low, weight_high = pair_weights(mass_ref[plane], mass_ref[plane + 1])
        allowed = jnp.maximum(allow_ref[plane], allow_ref[plane + 1])
        closing = jnp.maximum(low - high, 0.0)
        push = allowed * closing * jnp.tanh(wide * closing)
        u_ref[plane] = low - weight_low * push
        u_ref[plane + 1] = high + weight_high * push
    for k in range(EXT):
        next_ref[k] = u_ref[1 + k]
    for field, (place, planes) in enumerate(edge_layout(X_LEFT)[0]):
        for k in range(planes):
            for edge_ref, plane in ((xlo_ref, k), (xhi_ref, EXT - planes + k)):
                if field == 0:
                    edge_ref[place + k] = next_ref[plane]
                elif field == 1:
                    edge_ref[place + k] = own_mass_ref[plane]
                else:
                    edge_ref[place + k] = bits_ref[field - 2, plane]
    sends = [
        pltpu.make_async_copy(xlo_ref, xlo_hbm, sems.at[0]),
        pltpu.make_async_copy(xhi_ref, xhi_hbm, sems.at[1]),
    ]
    for send in sends:
        send.start()
    energy = jnp.zeros((PAD, NZ), f32)
    for k in range(EXT):
        u = next_ref[k]
        energy = energy + own_mass_ref[k] * u * u
    mine = fold(energy)
    half = NZ // 2
    lane = lax.broadcasted_iota(jnp.int32, (1, NZ), 1)
    local = carry_ref[2:3, :] + mine + carry_ref[4:5, :]
    number = carry_ref[5:6, :]
    local = jnp.where(lane < half, local + pltpu.roll(local, half, 1), number + pltpu.roll(number, half, 1))
    out_ref[...] = carry_ref[...]
    out_ref[3:4, :] = mine
    rows_ref[...] = jnp.broadcast_to(local, (DEVICES, NZ))
    for send in sends:
        send.wait()


def first(carry, own, mass, allow, bits, below, above):
    edge = (edge_layout(X_LEFT)[1], PAD, NZ)
    return pl.pallas_call(
        first_kernel,
        in_specs=[VMEM] * 7,
        out_specs=[VMEM] * 3 + [ANY] * 2,
        out_shape=[shape(DEVICES, NZ), shape(CARRY, NZ), shape(EXT, PAD, NZ), far(*edge), far(*edge)],
        scratch_shapes=[pltpu.VMEM((EXT + 2, PAD, NZ), f32)] * 3
        + [pltpu.VMEM(edge, f32)] * 2
        + [pltpu.SemaphoreType.DMA((2,))],
        compiler_params=GRANT,
        name="first",
    )(carry, own, mass, allow, bits, below, above)


def pair_weights(mass_low, mass_high):
    reduced = mass_low * mass_high / jnp.maximum(mass_low + mass_high, 1.0)
    return reduced / jnp.maximum(mass_low, 1.0), reduced / jnp.maximum(mass_high, 1.0)


def join_kernel(
    carry_ref, own_ref, mass_ref, own_bits_ref, below_ref, above_ref, u_ref, weight_ref, all_mass_ref, bits_ref, both_ref, *, left, first_step
):
    for field, (place, planes) in enumerate(edge_layout(left)[0]):
        for k in range(planes):
            low, high = below_ref[place + k], above_ref[place + k]
            below, above = left - planes + k, left + EXT + k
            if field == 0:
                u_ref[below], u_ref[above] = low, high
            elif field == 1:
                all_mass_ref[below], all_mass_ref[above] = low, high
            else:
                bits_ref[field - 2, below], bits_ref[field - 2, above] = low, high
        for k in range(left - planes):
            bits_ref[field - 2, k] = jnp.zeros((PAD, NZ), f32)
            bits_ref[field - 2, full_planes(left) - 1 - k] = jnp.zeros((PAD, NZ), f32)
    for k in range(EXT):
        u_ref[left + k] = own_ref[k]
        all_mass_ref[left + k] = mass_ref[k]
        for j in range(left):
            bits_ref[j, left + k] = own_bits_ref[j, k]
    for plane in range(full_planes(left) - 1):
        both_ref[0, plane], both_ref[1, plane] = pair_weights(all_mass_ref[plane], all_mass_ref[plane + 1])
    for j in range(left):
        start = whole(carry_ref, START_ROW + first_step + 2 * j)
        for k in range(pair_count(left)):
            plane = start + 2 * k
            allowed = jnp.maximum(bits_ref[j, plane], bits_ref[j, plane + 1])
            weight_ref[j, 0, k] = allowed * both_ref[0, plane]
            weight_ref[j, 1, k] = allowed * both_ref[1, plane]


def join(carry, own, mass, bits, below, above, left, first_step):
    def body(*refs):
        join_kernel(*refs, left=left, first_step=first_step)

    full, pairs = full_planes(left), pair_count(left)
    return pl.pallas_call(
        body,
        in_specs=[VMEM] * 6,
        out_specs=[VMEM] * 2,
        out_shape=[shape(full, PAD, NZ), shape(left, 2, pairs, PAD, NZ)],
        scratch_shapes=[
            pltpu.VMEM((full, PAD, NZ), f32),
            pltpu.VMEM((left, full, PAD, NZ), f32),
            pltpu.VMEM((2, full, PAD, NZ), f32),
        ],
        compiler_params=GRANT,
        name="join",
    )(carry, own, mass, bits, below, above)


def next_scale(received_ref, carry_ref, step):
    sums = jnp.sum(received_ref[...], axis=0, keepdims=True)
    scale = carry_ref[0:1, :]
    if step == 0:
        lane = lax.broadcasted_iota(jnp.int32, (1, NZ), 1)
        energy = jnp.sum(jnp.where(lane < NZ // 2, sums, 0.0), axis=1, keepdims=True)
        total = jnp.sum(jnp.where(lane < NZ // 2, 0.0, sums), axis=1, keepdims=True)
        total = jnp.broadcast_to(total, (1, NZ))
    else:
        energy = jnp.sum(sums, axis=1, keepdims=True)
        total = carry_ref[1:2, :]
    speed = scale * jnp.sqrt(jnp.broadcast_to(energy, (1, NZ)))
    factor = jnp.sqrt(carry_ref[HEAT_ROW + step : HEAT_ROW + step + 1, :] * total / (speed * speed + excess_coupling))
    return jnp.minimum(scale * factor, SCALE_CAP), total


def step_kernel(received_ref, carry_ref, u_in_ref, weight_ref, mass_ref, u_ref, rows_ref, out_ref, *, step, left):
    start = whole(carry_ref, START_ROW + step)
    scale, total = next_scale(received_ref, carry_ref, step - 1)
    wide = jnp.broadcast_to(scale, (PAD, NZ))
    turn = left - (STEPS + 1 - step) // 2
    u_ref[0] = u_in_ref[0]
    u_ref[full_planes(left) - 1] = u_in_ref[full_planes(left) - 1]
    for k in range(pair_count(left)):
        plane = start + 2 * k
        low, high = u_in_ref[plane], u_in_ref[plane + 1]
        closing = jnp.maximum(low - high, 0.0)
        push = closing * jnp.tanh(wide * closing)
        u_ref[plane] = low - weight_ref[turn, 0, k] * push
        u_ref[plane + 1] = high + weight_ref[turn, 1, k] * push
    energy = jnp.zeros((PAD, NZ), f32)
    for k in range(EXT):
        u = u_ref[left + k]
        energy = energy + mass_ref[k] * u * u
    mine = fold(energy)
    other = carry_ref[4:5, :] if step % 2 == 0 else carry_ref[3:4, :]
    out_ref[...] = carry_ref[...]
    out_ref[0:1, :] = scale
    out_ref[1:2, :] = total
    row = 3 if step % 2 == 0 else 4
    out_ref[row : row + 1, :] = mine
    rows_ref[...] = jnp.broadcast_to(carry_ref[2:3, :] + mine + other, (DEVICES, NZ))


def collide(step, received, carry, u, weight, mass):
    left, _ = place_of(step)

    def body(*refs):
        step_kernel(*refs, step=step, left=left)

    return pl.pallas_call(
        body,
        in_specs=[VMEM] * 5,
        out_specs=[VMEM] * 3,
        out_shape=[shape(full_planes(left), PAD, NZ), shape(DEVICES, NZ), shape(CARRY, NZ)],
        compiler_params=GRANT,
        name="collide",
    )(received, carry, u, weight, mass)


def turn_kernel(carry_ref, v_ref, count_ref, spin_ref, w_hbm, w_ref, sems):
    shifts = [whole(carry_ref, SHIFT_ROW + step) for step in range(STEPS)]

    def plane(i, carry):
        real = jnp.ones((EXT, NZ), f32)
        parts = [jnp.zeros((EXT, NZ), f32)] * 3
        for step in range(STEPS):
            spin = pltpu.roll(spin_ref[step, i], shifts[step], 1)
            tangent = jnp.where((spin & 1) == 0, HALF_TAN, -HALF_TAN)
            on_x, on_y = spin < 2, spin < 4
            x, y, z = parts

            def pick(first, second, third):
                return tangent * jnp.where(on_x, first, jnp.where(on_y, second, third))

            real, parts = (
                real - pick(x, y, z),
                [x + pick(real, z, -y), y + pick(-z, real, x), z + pick(y, -x, real)],
            )
        x, y, z = parts
        unit = BIG * TURN_NORM
        xx, yy, zz, rr = x * x, y * y, z * z, real * real
        rows = [
            [(rr + xx) - (yy + zz), 2.0 * (x * y - real * z), 2.0 * (x * z + real * y)],
            [2.0 * (x * y + real * z), (rr + yy) - (xx + zz), 2.0 * (y * z - real * x)],
            [2.0 * (x * z - real * y), 2.0 * (y * z + real * x), (rr + zz) - (xx + yy)],
        ]
        rows = [[unit * value for value in row] for row in rows]
        counts = pltpu.roll(count_ref[i], shifts[0], 1)
        inverse = 1.0 / jnp.maximum(counts.astype(f32), 1.0)
        values = [
            [
                jnp.where(counts > slot, pltpu.roll(v_ref[member, slot, i], shifts[0], 1), 0.0)
                for slot in range(SLOTS)
            ]
            for member in range(3)
        ]
        mean = []
        for member in range(3):
            moment = values[member][0]
            for slot in range(1, SLOTS):
                moment = moment + values[member][slot]
            mean.append(moment * inverse)
        for slot in range(SLOTS):
            rest = [values[member][slot] - mean[member] for member in range(3)]
            for member in range(3):
                turned = rows[member][0] * rest[0] + rows[member][1] * rest[1] + rows[member][2] * rest[2]
                w_ref[member, slot, i] = turned
        send(i).start()
        return carry

    def send(i):
        part = pl.ds(i, 1)
        return pltpu.make_async_copy(w_ref.at[:, :, part], w_hbm.at[:, :, part], sems.at[i])

    lax.fori_loop(0, EXT, plane, 0)
    for i in range(EXT):
        send(i).wait()


def turn(carry, v, counts, spin):
    return pl.pallas_call(
        turn_kernel,
        in_specs=[VMEM] * 4,
        out_specs=ANY,
        out_shape=far(3, SLOTS, EXT, EXT, NZ),
        scratch_shapes=[pltpu.VMEM((3, SLOTS, EXT, EXT, NZ), f32), pltpu.SemaphoreType.DMA((EXT,))],
        compiler_params=GRANT,
        name="turn",
    )(carry, v, counts, spin)


def finish_kernel(received_ref, carry_ref, ux_ref, uy_ref, uz_ref, mass_ref, w_ref, v_ref):
    member = pl.program_id(0)
    scale, _ = next_scale(received_ref, carry_ref, STEPS - 1)
    wide = jnp.broadcast_to(scale, (EXT, NZ))

    def write(mean_of):
        for i in range(EXT):
            counts = mass_ref[i, 0:EXT, :]
            mean = mean_of(i)
            for slot in range(SLOTS):
                v_ref[0, slot, i] = jnp.where(counts > slot, wide * (mean + w_ref[0, slot, i]), 0.0)

    @pl.when(member == 0)
    def _():
        write(lambda i: ux_ref[X_LEFT + i, 0:EXT, :])

    @pl.when(member == 1)
    def _():
        write(lambda i: uy_ref[pl.ds(Y_LEFT * PAD + i, EXT, stride=PAD), :])

    @pl.when(member == 2)
    def _():
        write(lambda i: uz_ref[i, 0:EXT, :])


def finish(received, carry, ux, uy, uz, mass, w):
    part = pl.BlockSpec((1, SLOTS, EXT, EXT, NZ), lambda c: (c, 0, 0, 0, 0))
    return pl.pallas_call(
        finish_kernel,
        grid=(3,),
        in_specs=[VMEM] * 6 + [part],
        out_specs=part,
        out_shape=shape(3, SLOTS, EXT, EXT, NZ),
        compiler_params=GRANT,
        name="finish",
    )(received, carry, ux, uy.reshape(full_planes(Y_LEFT) * PAD, NZ), uz, mass, w)


def exchange(low_edge, high_edge, axis):
    count = lax.axis_size(axis)
    down = [(source, (source - 1) % count) for source in range(count)]
    up = [(source, (source + 1) % count) for source in range(count)]
    return lax.ppermute(low_edge, axis, down), lax.ppermute(high_edge, axis, up)


def sum_over_devices(rows):
    return lax.all_to_all(rows, ("bx", "by"), 0, 0, tiled=True)


def per_device(v, counts, spin, flags, parity, shifts, heat):
    ux, mass, allow, uy, uz, low, high, carry = prep(shifts, parity, heat, v, counts, flags)
    carry, v, counts, spin, flags = lax.optimization_barrier((carry, v, counts, spin, flags))
    above, below = exchange(low, high, "bx")
    bits, uy, y_mass, y_bits, ylo, yhi = spread(carry, mass, uy, flags)
    y_above, y_below = exchange(ylo, yhi, "by")
    w = turn(carry, v, counts, spin)
    below, above, w = lax.optimization_barrier((below, above, w))
    rows, carry, ux, xlo, xhi = first(carry, ux, mass, allow, bits, below, above)
    received = sum_over_devices(rows)
    x_above, x_below = exchange(xlo, xhi, "bx")
    received, carry, uy = lax.optimization_barrier((received, carry, uy))
    uy, y_weights = join(carry, uy, y_mass, y_bits, y_below, y_above, Y_LEFT, 1)
    for step in range(1, STEPS):
        if step % 2 == 0:
            ux, rows, carry = collide(step, received, carry, ux, x_weights, mass)
        else:
            uy, rows, carry = collide(step, received, carry, uy, y_weights, y_mass)
        received = sum_over_devices(rows)
        if step == 1:
            received, carry, ux = lax.optimization_barrier((received, carry, ux))
            ux, x_weights = join(carry, ux, mass, bits, x_below, x_above, X_LEFT, 2)
    return finish(received, carry, ux, uy, uz, mass, w)


def solution(mesh):
    return jax.shard_map(
        per_device,
        mesh=mesh,
        in_specs=(
            P(None, None, "bx", "by", None),
            P("bx", "by", None),
            P(None, "bx", "by", None),
            P(None, "bx", "by", None),
            P(),
            P(),
            P(),
        ),
        out_specs=P(None, None, "bx", "by", None),
        check_vma=False,
    )
```

```python
import math

import jax
import jax.numpy as jnp
from jax import lax
from jax.experimental import pallas as pl
from jax.experimental.pallas import tpu as pltpu
from jax.sharding import PartitionSpec as P

STEPS = 12
HALF = STEPS // 2
SLOTS = 6
EXT = 15
PAD = 16
CHUNK = 3
TURN_UNROLL = 5
NZ = 128
DEVICES = 128
X_LEFT = HALF - 1
Y_LEFT = HALF
HEAT_ROW = 8
START_ROW = HEAT_ROW + PAD
SHIFT_ROW = START_ROW + PAD
CARRY = SHIFT_ROW + PAD

turn_angle = 130.0 * math.pi / 180.0
excess_coupling = 1e-06
BIG = 2.0**46
SCALE_CAP = 3e38
HALF_TAN = math.tan(turn_angle / 2.0)
TURN_NORM = math.cos(turn_angle / 2.0) ** (2 * STEPS)

VMEM = pl.BlockSpec(memory_space=pltpu.VMEM)
SMEM = pl.BlockSpec(memory_space=pltpu.SMEM)
ANY = pl.BlockSpec(memory_space=pl.ANY)
f32 = jnp.float32
GRANT = pltpu.CompilerParams(vmem_limit_bytes=12 * 2**20)


def shape(*dims):
    return jax.ShapeDtypeStruct(dims, f32)


def far(*dims):
    return pltpu.HBM(dims, f32)


def later_shifts(shift_ref, step):
    total = jnp.int32(0)
    for later in range(step, STEPS):
        total = total + shift_ref[later]
    return lax.rem(total, jnp.int32(NZ))


def edge_layout(left):
    counts = [left, left] + [left - k for k in range(left)]
    starts = [sum(counts[:k]) for k in range(len(counts))]
    return list(zip(starts, counts)), sum(counts)


def full_planes(left):
    return EXT + 2 * left


def pair_count(left):
    return (full_planes(left) - 1) // 2


def whole(carry_ref, row):
    return carry_ref[row : row + 1, :][0, 0].astype(jnp.int32)


def place_of(step):
    return (X_LEFT, "bx") if step % 2 == 0 else (Y_LEFT, "by")


def fold(values):
    return jnp.sum(values, axis=0, keepdims=True)


def prep_kernel(
    shift_hbm, parity_hbm, heat_hbm, v_hbm, count_hbm, flag_hbm,
    ux_ref, mass_ref, allow_ref, uy_ref, uz_ref, low_ref, high_ref, base_ref,
    shift_ref, parity_ref, heat_ref, v_ref, count_ref, flag_ref, sems, chunk_sems,
):
    fetches = [
        pltpu.make_async_copy(shift_hbm, shift_ref, sems.at[0]),
        pltpu.make_async_copy(count_hbm, count_ref, sems.at[1]),
        pltpu.make_async_copy(flag_hbm.at[0], flag_ref, sems.at[2]),
        pltpu.make_async_copy(parity_hbm, parity_ref, sems.at[3]),
        pltpu.make_async_copy(heat_hbm, heat_ref, sems.at[4]),
    ]
    chunks = [
        pltpu.make_async_copy(
            v_hbm.at[:, :, pl.ds(CHUNK * c, CHUNK)], v_ref.at[:, :, pl.ds(CHUNK * c, CHUNK)], chunk_sems.at[c]
        )
        for c in range(EXT // CHUNK)
    ]
    for fetch in fetches + chunks:
        fetch.start()
    for fetch in fetches:
        fetch.wait()
    shift = later_shifts(shift_ref, 0)
    zero_row = jnp.zeros((EXT, 1, NZ), f32)
    for array_ref in (ux_ref, mass_ref, allow_ref, uy_ref, uz_ref):
        array_ref[0:EXT, EXT:PAD, :] = zero_row
    uy_ref[EXT] = jnp.zeros((PAD, NZ), f32)

    thermal = energy_y = total = jnp.zeros((EXT, NZ), f32)
    for i in range(EXT):
        if i % CHUNK == 0:
            chunks[i // CHUNK].wait()
        counts = count_ref[i]
        mass = counts.astype(f32)
        inverse = 1.0 / jnp.maximum(mass, 1.0)
        mean = []
        for member in range(3):
            values = [
                jnp.where(counts > slot, v_ref[member, slot, i] * BIG, 0.0) for slot in range(SLOTS)
            ]
            moment = values[0]
            for slot in range(1, SLOTS):
                moment = moment + values[slot]
            middle = moment * inverse
            mean.append(middle)
            for slot in range(SLOTS):
                rest = jnp.where(counts > slot, values[slot] - middle, 0.0)
                thermal = thermal + rest * rest
        thermal = thermal + mass * mean[2] * mean[2]
        energy_y = energy_y + mass * mean[1] * mean[1]
        total = total + mass
        ux_ref[i, 0:EXT, :] = pltpu.roll(mean[0], shift, 1)
        mass_ref[i, 0:EXT, :] = pltpu.roll(mass, shift, 1)
        allow_ref[i, 0:EXT, :] = pltpu.roll(flag_ref[i].astype(f32), shift, 1)
        uy_ref[i, 0:EXT, :] = pltpu.roll(mean[1], shift, 1)
        uz_ref[i, 0:EXT, :] = pltpu.roll(mean[2], shift, 1)
    base_ref[...] = jnp.zeros((CARRY, NZ), f32)
    for step in range(STEPS):
        left, brick_axis = place_of(step)
        start = lower_start(parity_ref, step, brick_axis, left)
        base_ref[HEAT_ROW + step : HEAT_ROW + step + 1, :] = jnp.full((1, NZ), 3.0 * heat_ref[step], f32)
        base_ref[START_ROW + step : START_ROW + step + 1, :] = jnp.full((1, NZ), start.astype(f32), f32)
        later = later_shifts(shift_ref, step)
        base_ref[SHIFT_ROW + step : SHIFT_ROW + step + 1, :] = jnp.full((1, NZ), later.astype(f32), f32)
    base_ref[0:1, :] = jnp.full((1, NZ), 1.0 / BIG, f32)
    base_ref[2:3, :] = fold(thermal)
    base_ref[4:5, :] = fold(energy_y)
    base_ref[5:6, :] = fold(total)
    for field, array_ref in enumerate((ux_ref, mass_ref, allow_ref)):
        low_ref[field] = array_ref[0]
        high_ref[field] = array_ref[EXT - 1]


def prep(shifts, parity, heat, v, counts, flags):
    edge = shape(3, PAD, NZ)
    return pl.pallas_call(
        prep_kernel,
        in_specs=[ANY] * 6,
        out_specs=[VMEM] * 8,
        out_shape=[shape(EXT, PAD, NZ)] * 3 + [shape(PAD, PAD, NZ), shape(EXT, PAD, NZ), edge, edge, shape(CARRY, NZ)],
        scratch_shapes=[
            pltpu.SMEM((STEPS,), jnp.int32),
            pltpu.SMEM((STEPS,), jnp.int32),
            pltpu.SMEM((STEPS,), f32),
            pltpu.VMEM((3, SLOTS, EXT, EXT, NZ), f32),
            pltpu.VMEM((EXT, EXT, NZ), jnp.int32),
            pltpu.VMEM((EXT, EXT, NZ), jnp.int32),
            pltpu.SemaphoreType.DMA((5,)),
            pltpu.SemaphoreType.DMA((EXT // CHUNK,)),
        ],
        compiler_params=GRANT,
        name="prep",
    )(*[pltpu.with_memory_space_constraint(array, pltpu.HBM) for array in (shifts, parity, heat, v, counts, flags)])


def spread_kernel(carry_ref, mass_ref, uy_ref, flag_ref, bits_ref, own_ref, y_mass_ref, y_bits_ref, low_ref, high_ref, turn_ref):
    bits_ref[:, :, EXT:PAD, :] = jnp.zeros((X_LEFT, EXT, 1, NZ), f32)
    for step in range(1, STEPS):
        later = whole(carry_ref, SHIFT_ROW + step)
        for i in range(EXT):
            bits = pltpu.roll(flag_ref[step, i].astype(f32), later, 1)
            if step % 2 == 0:
                bits_ref[step // 2 - 1, i, 0:EXT, :] = bits
            else:
                turn_ref[step // 2, i * PAD : i * PAD + EXT, :] = bits
    keep = lax.broadcasted_iota(jnp.int32, (PAD, NZ), 0) < EXT
    for i in range(EXT):
        turn_ref[HALF, i * PAD : (i + 1) * PAD, :] = mass_ref[i]
    for field, (place, planes) in enumerate(edge_layout(Y_LEFT)[0]):
        for y in range(EXT):
            line = pl.ds(y, PAD, stride=PAD)
            if field == 0:
                rows = own_ref[y] = jnp.where(keep, uy_ref[line, :], 0.0)
            elif field == 1:
                rows = y_mass_ref[y] = jnp.where(keep, turn_ref[HALF, line, :], 0.0)
            else:
                rows = y_bits_ref[field - 2, y] = jnp.where(keep, turn_ref[field - 2, line, :], 0.0)
            if y < planes:
                low_ref[place + y] = rows
            if y >= EXT - planes:
                high_ref[place + y - (EXT - planes)] = rows


def spread(carry, mass, uy, flags):
    edge = shape(edge_layout(Y_LEFT)[1], PAD, NZ)
    plane = shape(EXT, PAD, NZ)
    return pl.pallas_call(
        spread_kernel,
        in_specs=[VMEM] * 4,
        out_specs=[VMEM] * 6,
        out_shape=[shape(X_LEFT, EXT, PAD, NZ), plane, plane, shape(Y_LEFT, EXT, PAD, NZ), edge, edge],
        scratch_shapes=[pltpu.VMEM((HALF + 1, PAD * PAD, NZ), f32)],
        compiler_params=GRANT,
        name="spread",
    )(carry, mass, uy.reshape(PAD * PAD, NZ), flags)


def lower_start(parity_ref, step, brick_axis, halo):
    return lax.rem(parity_ref[step] + lax.axis_index(brick_axis) * EXT + halo, jnp.int32(2))


def first_kernel(
    carry_ref, own_ref, own_mass_ref, own_allow_ref, bits_ref, below_ref, above_ref,
    rows_ref, out_ref, next_ref, xlo_hbm, xhi_hbm, u_ref, mass_ref, allow_ref, xlo_ref, xhi_ref, sems,
):
    layout, edge_count = edge_layout(X_LEFT)
    edges = ((xlo_ref, xlo_hbm, 0), (xhi_ref, xhi_hbm, 1))
    for field, (place, planes) in enumerate(layout):
        for k in range(planes):
            for edge_ref, plane in ((xlo_ref, k), (xhi_ref, EXT - planes + k)):
                if field == 1:
                    edge_ref[place + k] = own_mass_ref[plane]
                elif field > 1:
                    edge_ref[place + k] = bits_ref[field - 2, plane]
    fixed, moved = pl.ds(X_LEFT, edge_count - X_LEFT), pl.ds(0, X_LEFT)
    sends = [pltpu.make_async_copy(src.at[fixed], dst.at[fixed], sems.at[k]) for src, dst, k in edges]
    for send in sends:
        send.start()
    for field, (all_ref, mine_ref) in enumerate(
        ((u_ref, own_ref), (mass_ref, own_mass_ref), (allow_ref, own_allow_ref))
    ):
        all_ref[0] = below_ref[field]
        all_ref[EXT + 1] = above_ref[field]
        for k in range(EXT):
            all_ref[1 + k] = mine_ref[k]
    start = whole(carry_ref, START_ROW)
    wide = jnp.broadcast_to(carry_ref[0:1, :], (PAD, NZ))
    for k in range((EXT + 1) // 2):
        plane = start + 2 * k
        low, high = u_ref[plane], u_ref[plane + 1]
        weight_low, weight_high = pair_weights(mass_ref[plane], mass_ref[plane + 1])
        allowed = jnp.maximum(allow_ref[plane], allow_ref[plane + 1])
        closing = jnp.maximum(low - high, 0.0)
        push = allowed * closing * jnp.tanh(wide * closing)
        u_ref[plane] = low - weight_low * push
        u_ref[plane + 1] = high + weight_high * push
    for k in range(EXT):
        next_ref[k] = u_ref[1 + k]
    for k in range(X_LEFT):
        xlo_ref[k] = u_ref[1 + k]
        xhi_ref[k] = u_ref[1 + EXT - X_LEFT + k]
    for src, dst, k in edges:
        sends.append(pltpu.make_async_copy(src.at[moved], dst.at[moved], sems.at[2 + k]))
        sends[-1].start()
    energy = jnp.zeros((PAD, NZ), f32)
    for k in range(EXT):
        u = next_ref[k]
        energy = energy + own_mass_ref[k] * u * u
    mine = fold(energy)
    half = NZ // 2
    lane = lax.broadcasted_iota(jnp.int32, (1, NZ), 1)
    local = carry_ref[2:3, :] + mine + carry_ref[4:5, :]
    number = carry_ref[5:6, :]
    local = jnp.where(lane < half, local + pltpu.roll(local, half, 1), number + pltpu.roll(number, half, 1))
    out_ref[...] = carry_ref[...]
    out_ref[3:4, :] = mine
    rows_ref[...] = jnp.broadcast_to(local, (DEVICES, NZ))
    for send in sends:
        send.wait()


def first(carry, own, mass, allow, bits, below, above):
    edge = (edge_layout(X_LEFT)[1], PAD, NZ)
    return pl.pallas_call(
        first_kernel,
        in_specs=[VMEM] * 7,
        out_specs=[VMEM] * 3 + [ANY] * 2,
        out_shape=[shape(DEVICES, NZ), shape(CARRY, NZ), shape(EXT, PAD, NZ), far(*edge), far(*edge)],
        scratch_shapes=[pltpu.VMEM((EXT + 2, PAD, NZ), f32)] * 3
        + [pltpu.VMEM(edge, f32)] * 2
        + [pltpu.SemaphoreType.DMA((4,))],
        compiler_params=GRANT,
        name="first",
    )(carry, own, mass, allow, bits, below, above)


def pair_weights(mass_low, mass_high):
    reduced = mass_low * mass_high / jnp.maximum(mass_low + mass_high, 1.0)
    return reduced / jnp.maximum(mass_low, 1.0), reduced / jnp.maximum(mass_high, 1.0)


def join_kernel(
    carry_ref, own_ref, mass_ref, own_bits_ref, below_ref, above_ref, u_ref, weight_ref, all_mass_ref, bits_ref, both_ref, *, left, first_step
):
    for field, (place, planes) in enumerate(edge_layout(left)[0]):
        for k in range(planes):
            low, high = below_ref[place + k], above_ref[place + k]
            below, above = left - planes + k, left + EXT + k
            if field == 0:
                u_ref[below], u_ref[above] = low, high
            elif field == 1:
                all_mass_ref[below], all_mass_ref[above] = low, high
            else:
                bits_ref[field - 2, below], bits_ref[field - 2, above] = low, high
        for k in range(left - planes):
            bits_ref[field - 2, k] = jnp.zeros((PAD, NZ), f32)
            bits_ref[field - 2, full_planes(left) - 1 - k] = jnp.zeros((PAD, NZ), f32)
    for k in range(EXT):
        u_ref[left + k] = own_ref[k]
        all_mass_ref[left + k] = mass_ref[k]
        for j in range(left):
            bits_ref[j, left + k] = own_bits_ref[j, k]
    for plane in range(full_planes(left) - 1):
        both_ref[0, plane], both_ref[1, plane] = pair_weights(all_mass_ref[plane], all_mass_ref[plane + 1])
    for j in range(left):
        start = whole(carry_ref, START_ROW + first_step + 2 * j)
        for k in range(pair_count(left)):
            plane = start + 2 * k
            allowed = jnp.maximum(bits_ref[j, plane], bits_ref[j, plane + 1])
            weight_ref[j, 0, k] = allowed * both_ref[0, plane]
            weight_ref[j, 1, k] = allowed * both_ref[1, plane]


def join(carry, own, mass, bits, below, above, left, first_step):
    def body(*refs):
        join_kernel(*refs, left=left, first_step=first_step)

    full, pairs = full_planes(left), pair_count(left)
    return pl.pallas_call(
        body,
        in_specs=[VMEM] * 6,
        out_specs=[VMEM] * 2,
        out_shape=[shape(full, PAD, NZ), shape(left, 2, pairs, PAD, NZ)],
        scratch_shapes=[
            pltpu.VMEM((full, PAD, NZ), f32),
            pltpu.VMEM((left, full, PAD, NZ), f32),
            pltpu.VMEM((2, full, PAD, NZ), f32),
        ],
        compiler_params=GRANT,
        name="join",
    )(carry, own, mass, bits, below, above)


def next_scale(received_ref, carry_ref, step):
    sums = jnp.sum(received_ref[...], axis=0, keepdims=True)
    scale = carry_ref[0:1, :]
    if step == 0:
        lane = lax.broadcasted_iota(jnp.int32, (1, NZ), 1)
        energy = jnp.sum(jnp.where(lane < NZ // 2, sums, 0.0), axis=1, keepdims=True)
        total = jnp.sum(jnp.where(lane < NZ // 2, 0.0, sums), axis=1, keepdims=True)
        total = jnp.broadcast_to(total, (1, NZ))
    else:
        energy = jnp.sum(sums, axis=1, keepdims=True)
        total = carry_ref[1:2, :]
    speed = scale * jnp.sqrt(jnp.broadcast_to(energy, (1, NZ)))
    factor = jnp.sqrt(carry_ref[HEAT_ROW + step : HEAT_ROW + step + 1, :] * total / (speed * speed + excess_coupling))
    return jnp.minimum(scale * factor, SCALE_CAP), total


def step_kernel(received_ref, carry_ref, u_in_ref, weight_ref, mass_ref, u_ref, rows_ref, out_ref, *, step, left):
    start = whole(carry_ref, START_ROW + step)
    scale, total = next_scale(received_ref, carry_ref, step - 1)
    wide = jnp.broadcast_to(scale, (PAD, NZ))
    turn = left - (STEPS + 1 - step) // 2
    u_ref[0] = u_in_ref[0]
    u_ref[full_planes(left) - 1] = u_in_ref[full_planes(left) - 1]
    for k in range(pair_count(left)):
        plane = start + 2 * k
        low, high = u_in_ref[plane], u_in_ref[plane + 1]
        closing = jnp.maximum(low - high, 0.0)
        push = closing * jnp.tanh(wide * closing)
        u_ref[plane] = low - weight_ref[turn, 0, k] * push
        u_ref[plane + 1] = high + weight_ref[turn, 1, k] * push
    energy = jnp.zeros((PAD, NZ), f32)
    for k in range(EXT):
        u = u_ref[left + k]
        energy = energy + mass_ref[k] * u * u
    mine = fold(energy)
    other = carry_ref[4:5, :] if step % 2 == 0 else carry_ref[3:4, :]
    out_ref[...] = carry_ref[...]
    out_ref[0:1, :] = scale
    out_ref[1:2, :] = total
    row = 3 if step % 2 == 0 else 4
    out_ref[row : row + 1, :] = mine
    rows_ref[...] = jnp.broadcast_to(carry_ref[2:3, :] + mine + other, (DEVICES, NZ))


def collide(step, received, carry, u, weight, mass):
    left, _ = place_of(step)

    def body(*refs):
        step_kernel(*refs, step=step, left=left)

    return pl.pallas_call(
        body,
        in_specs=[VMEM] * 5,
        out_specs=[VMEM] * 3,
        out_shape=[shape(full_planes(left), PAD, NZ), shape(DEVICES, NZ), shape(CARRY, NZ)],
        compiler_params=GRANT,
        name="collide",
    )(received, carry, u, weight, mass)


def turn_kernel(carry_ref, v_ref, count_ref, spin_ref, w_hbm, w_ref, sems):
    shifts = [whole(carry_ref, SHIFT_ROW + step) for step in range(STEPS)]

    def plane(i, carry):
        real = jnp.ones((EXT, NZ), f32)
        parts = [jnp.zeros((EXT, NZ), f32)] * 3
        for step in range(STEPS):
            spin = pltpu.roll(spin_ref[step, i], shifts[step], 1)
            tangent = jnp.where((spin & 1) == 0, HALF_TAN, -HALF_TAN)
            on_x, on_y = spin < 2, spin < 4
            x, y, z = parts

            def pick(first, second, third):
                return tangent * jnp.where(on_x, first, jnp.where(on_y, second, third))

            real, parts = (
                real - pick(x, y, z),
                [x + pick(real, z, -y), y + pick(-z, real, x), z + pick(y, -x, real)],
            )
        x, y, z = parts
        unit = BIG * TURN_NORM
        xx, yy, zz, rr = x * x, y * y, z * z, real * real
        rows = [
            [(rr + xx) - (yy + zz), 2.0 * (x * y - real * z), 2.0 * (x * z + real * y)],
            [2.0 * (x * y + real * z), (rr + yy) - (xx + zz), 2.0 * (y * z - real * x)],
            [2.0 * (x * z - real * y), 2.0 * (y * z + real * x), (rr + zz) - (xx + yy)],
        ]
        rows = [[unit * value for value in row] for row in rows]
        counts = pltpu.roll(count_ref[i], shifts[0], 1)
        inverse = 1.0 / jnp.maximum(counts.astype(f32), 1.0)
        values = [
            [
                jnp.where(counts > slot, pltpu.roll(v_ref[member, slot, i], shifts[0], 1), 0.0)
                for slot in range(SLOTS)
            ]
            for member in range(3)
        ]
        mean = []
        for member in range(3):
            moment = values[member][0]
            for slot in range(1, SLOTS):
                moment = moment + values[member][slot]
            mean.append(moment * inverse)
        for slot in range(SLOTS):
            rest = [values[member][slot] - mean[member] for member in range(3)]
            for member in range(3):
                turned = rows[member][0] * rest[0] + rows[member][1] * rest[1] + rows[member][2] * rest[2]
                w_ref[member, slot, i] = turned
        send(i).start()
        return carry

    def send(i):
        part = pl.ds(i, 1)
        return pltpu.make_async_copy(w_ref.at[:, :, part], w_hbm.at[:, :, part], sems.at[i])

    lax.fori_loop(0, EXT, plane, 0, unroll=TURN_UNROLL)
    for i in range(EXT):
        send(i).wait()


def turn(carry, v, counts, spin):
    return pl.pallas_call(
        turn_kernel,
        in_specs=[VMEM] * 4,
        out_specs=ANY,
        out_shape=far(3, SLOTS, EXT, EXT, NZ),
        scratch_shapes=[pltpu.VMEM((3, SLOTS, EXT, EXT, NZ), f32), pltpu.SemaphoreType.DMA((EXT,))],
        compiler_params=GRANT,
        name="turn",
    )(carry, v, counts, spin)


def finish_kernel(received_ref, carry_ref, ux_ref, uy_ref, uz_ref, mass_ref, w_ref, v_hbm, v_ref, sems):
    scale, _ = next_scale(received_ref, carry_ref, STEPS - 1)
    wide = jnp.broadcast_to(scale, (EXT, NZ))
    sends = []
    for i in range(EXT):
        counts = mass_ref[i, 0:EXT, :]
        means = [
            ux_ref[X_LEFT + i, 0:EXT, :],
            uy_ref[pl.ds(Y_LEFT * PAD + i, EXT, stride=PAD), :],
            uz_ref[i, 0:EXT, :],
        ]
        for slot in range(SLOTS):
            live = counts > slot
            for member in range(3):
                v_ref[member, slot, i] = jnp.where(live, wide * (means[member] + w_ref[member, slot, i]), 0.0)
        if i % CHUNK == CHUNK - 1:
            part = pl.ds(i - (CHUNK - 1), CHUNK)
            sends.append(pltpu.make_async_copy(v_ref.at[:, :, part], v_hbm.at[:, :, part], sems.at[i // CHUNK]))
            sends[-1].start()
    for send in sends:
        send.wait()


def finish(received, carry, ux, uy, uz, mass, w):
    return pl.pallas_call(
        finish_kernel,
        in_specs=[VMEM] * 7,
        out_specs=ANY,
        out_shape=far(3, SLOTS, EXT, EXT, NZ),
        scratch_shapes=[pltpu.VMEM((3, SLOTS, EXT, EXT, NZ), f32), pltpu.SemaphoreType.DMA((EXT // CHUNK,))],
        compiler_params=GRANT,
        name="finish",
    )(received, carry, ux, uy.reshape(full_planes(Y_LEFT) * PAD, NZ), uz, mass, w)


def exchange(low_edge, high_edge, axis):
    count = lax.axis_size(axis)
    down = [(source, (source - 1) % count) for source in range(count)]
    up = [(source, (source + 1) % count) for source in range(count)]
    return lax.ppermute(low_edge, axis, down), lax.ppermute(high_edge, axis, up)


def sum_over_devices(rows):
    return lax.all_to_all(rows, ("bx", "by"), 0, 0, tiled=True)


def per_device(v, counts, spin, flags, parity, shifts, heat):
    ux, mass, allow, uy, uz, low, high, carry = prep(shifts, parity, heat, v, counts, flags)
    carry, v, counts, spin, flags = lax.optimization_barrier((carry, v, counts, spin, flags))
    above, below = exchange(low, high, "bx")
    bits, uy, y_mass, y_bits, ylo, yhi = spread(carry, mass, uy, flags)
    y_above, y_below = exchange(ylo, yhi, "by")
    w = turn(carry, v, counts, spin)
    below, above, w = lax.optimization_barrier((below, above, w))
    rows, carry, ux, xlo, xhi = first(carry, ux, mass, allow, bits, below, above)
    received = sum_over_devices(rows)
    x_above, x_below = exchange(xlo, xhi, "bx")
    received, carry, uy = lax.optimization_barrier((received, carry, uy))
    uy, y_weights = join(carry, uy, y_mass, y_bits, y_below, y_above, Y_LEFT, 1)
    for step in range(1, STEPS):
        if step % 2 == 0:
            ux, rows, carry = collide(step, received, carry, ux, x_weights, mass)
        else:
            uy, rows, carry = collide(step, received, carry, uy, y_weights, y_mass)
        received = sum_over_devices(rows)
        if step == 1:
            received, carry, ux = lax.optimization_barrier((received, carry, ux))
            ux, x_weights = join(carry, ux, mass, bits, x_below, x_above, X_LEFT, 2)
    return finish(received, carry, ux, uy, uz, mass, w)


def solution(mesh):
    return jax.shard_map(
        per_device,
        mesh=mesh,
        in_specs=(
            P(None, None, "bx", "by", None),
            P("bx", "by", None),
            P(None, "bx", "by", None),
            P(None, "bx", "by", None),
            P(),
            P(),
            P(),
        ),
        out_specs=P(None, None, "bx", "by", None),
        check_vma=False,
    )
```

```python
import math

import jax
import jax.numpy as jnp
from jax import lax
from jax.experimental import pallas as pl
from jax.experimental.pallas import tpu as pltpu
from jax.sharding import PartitionSpec as P

STEPS = 12
HALF = STEPS // 2
SLOTS = 6
EXT = 15
PAD = 16
CHUNK = 3
TURN_UNROLL = 5
NZ = 128
DEVICES = 128
X_LEFT = HALF - 1
Y_LEFT = HALF
HEAT_ROW = 8
START_ROW = HEAT_ROW + PAD
SHIFT_ROW = START_ROW + PAD
CARRY = SHIFT_ROW + PAD

turn_angle = 130.0 * math.pi / 180.0
excess_coupling = 1e-06
BIG = 2.0**46
SCALE_CAP = 3e38
HALF_TAN = math.tan(turn_angle / 2.0)
TURN_NORM = math.cos(turn_angle / 2.0) ** (2 * STEPS)

VMEM = pl.BlockSpec(memory_space=pltpu.VMEM)
SMEM = pl.BlockSpec(memory_space=pltpu.SMEM)
ANY = pl.BlockSpec(memory_space=pl.ANY)
f32 = jnp.float32
GRANT = pltpu.CompilerParams(vmem_limit_bytes=12 * 2**20)


def shape(*dims):
    return jax.ShapeDtypeStruct(dims, f32)


def far(*dims):
    return pltpu.HBM(dims, f32)


def later_shifts(shift_ref, step):
    total = jnp.int32(0)
    for later in range(step, STEPS):
        total = total + shift_ref[later]
    return lax.rem(total, jnp.int32(NZ))


def edge_layout(left):
    counts = [left, left] + [left - k for k in range(left)]
    starts = [sum(counts[:k]) for k in range(len(counts))]
    return list(zip(starts, counts)), sum(counts)


def full_planes(left):
    return EXT + 2 * left


def pair_count(left):
    return (full_planes(left) - 1) // 2


def whole(carry_ref, row):
    return carry_ref[row : row + 1, :][0, 0].astype(jnp.int32)


def place_of(step):
    return (X_LEFT, "bx") if step % 2 == 0 else (Y_LEFT, "by")


def fold(values):
    return jnp.sum(values, axis=0, keepdims=True)


def prep_kernel(
    shift_hbm, parity_hbm, heat_hbm, v_hbm, count_hbm, flag_hbm,
    ux_ref, mass_ref, allow_ref, uy_ref, uz_ref, low_ref, high_ref, base_ref,
    shift_ref, parity_ref, heat_ref, v_ref, count_ref, flag_ref, sems, chunk_sems,
):
    fetches = [
        pltpu.make_async_copy(shift_hbm, shift_ref, sems.at[0]),
        pltpu.make_async_copy(count_hbm, count_ref, sems.at[1]),
        pltpu.make_async_copy(flag_hbm.at[0], flag_ref, sems.at[2]),
        pltpu.make_async_copy(parity_hbm, parity_ref, sems.at[3]),
        pltpu.make_async_copy(heat_hbm, heat_ref, sems.at[4]),
    ]
    chunks = [
        pltpu.make_async_copy(
            v_hbm.at[:, :, pl.ds(CHUNK * c, CHUNK)], v_ref.at[:, :, pl.ds(CHUNK * c, CHUNK)], chunk_sems.at[c]
        )
        for c in range(EXT // CHUNK)
    ]
    for fetch in fetches + chunks:
        fetch.start()
    for fetch in fetches:
        fetch.wait()
    shift = later_shifts(shift_ref, 0)
    zero_row = jnp.zeros((EXT, 1, NZ), f32)
    for array_ref in (ux_ref, mass_ref, allow_ref, uy_ref, uz_ref):
        array_ref[0:EXT, EXT:PAD, :] = zero_row
    uy_ref[EXT] = jnp.zeros((PAD, NZ), f32)

    thermal = energy_y = total = jnp.zeros((EXT, NZ), f32)
    for i in range(EXT):
        if i % CHUNK == 0:
            chunks[i // CHUNK].wait()
        counts = count_ref[i]
        mass = counts.astype(f32)
        inverse = 1.0 / jnp.maximum(mass, 1.0)
        mean = []
        for member in range(3):
            values = [
                jnp.where(counts > slot, v_ref[member, slot, i] * BIG, 0.0) for slot in range(SLOTS)
            ]
            moment = values[0]
            for slot in range(1, SLOTS):
                moment = moment + values[slot]
            middle = moment * inverse
            mean.append(middle)
            for slot in range(SLOTS):
                rest = jnp.where(counts > slot, values[slot] - middle, 0.0)
                thermal = thermal + rest * rest
        thermal = thermal + mass * mean[2] * mean[2]
        energy_y = energy_y + mass * mean[1] * mean[1]
        total = total + mass
        ux_ref[i, 0:EXT, :] = pltpu.roll(mean[0], shift, 1)
        mass_ref[i, 0:EXT, :] = pltpu.roll(mass, shift, 1)
        allow_ref[i, 0:EXT, :] = pltpu.roll(flag_ref[i].astype(f32), shift, 1)
        uy_ref[i, 0:EXT, :] = pltpu.roll(mean[1], shift, 1)
        uz_ref[i, 0:EXT, :] = pltpu.roll(mean[2], shift, 1)
    base_ref[...] = jnp.zeros((CARRY, NZ), f32)
    for step in range(STEPS):
        left, brick_axis = place_of(step)
        start = lower_start(parity_ref, step, brick_axis, left)
        base_ref[HEAT_ROW + step : HEAT_ROW + step + 1, :] = jnp.full((1, NZ), 3.0 * heat_ref[step], f32)
        base_ref[START_ROW + step : START_ROW + step + 1, :] = jnp.full((1, NZ), start.astype(f32), f32)
        later = later_shifts(shift_ref, step)
        base_ref[SHIFT_ROW + step : SHIFT_ROW + step + 1, :] = jnp.full((1, NZ), later.astype(f32), f32)
    base_ref[0:1, :] = jnp.full((1, NZ), 1.0 / BIG, f32)
    base_ref[2:3, :] = fold(thermal)
    base_ref[4:5, :] = fold(energy_y)
    base_ref[5:6, :] = fold(total)
    for field, array_ref in enumerate((ux_ref, mass_ref, allow_ref)):
        low_ref[field] = array_ref[0]
        high_ref[field] = array_ref[EXT - 1]


def prep(shifts, parity, heat, v, counts, flags):
    edge = shape(3, PAD, NZ)
    return pl.pallas_call(
        prep_kernel,
        in_specs=[ANY] * 6,
        out_specs=[VMEM] * 8,
        out_shape=[shape(EXT, PAD, NZ)] * 3 + [shape(PAD, PAD, NZ), shape(EXT, PAD, NZ), edge, edge, shape(CARRY, NZ)],
        scratch_shapes=[
            pltpu.SMEM((STEPS,), jnp.int32),
            pltpu.SMEM((STEPS,), jnp.int32),
            pltpu.SMEM((STEPS,), f32),
            pltpu.VMEM((3, SLOTS, EXT, EXT, NZ), f32),
            pltpu.VMEM((EXT, EXT, NZ), jnp.int32),
            pltpu.VMEM((EXT, EXT, NZ), jnp.int32),
            pltpu.SemaphoreType.DMA((5,)),
            pltpu.SemaphoreType.DMA((EXT // CHUNK,)),
        ],
        compiler_params=GRANT,
        name="prep",
    )(*[pltpu.with_memory_space_constraint(array, pltpu.HBM) for array in (shifts, parity, heat, v, counts, flags)])


def spread_kernel(carry_ref, mass_ref, uy_ref, flag_ref, bits_ref, own_ref, y_mass_ref, y_bits_ref, low_ref, high_ref, turn_ref):
    bits_ref[:, :, EXT:PAD, :] = jnp.zeros((X_LEFT, EXT, 1, NZ), f32)
    for step in range(1, STEPS):
        later = whole(carry_ref, SHIFT_ROW + step)
        for i in range(EXT):
            bits = pltpu.roll(flag_ref[step, i].astype(f32), later, 1)
            if step % 2 == 0:
                bits_ref[step // 2 - 1, i, 0:EXT, :] = bits
            else:
                turn_ref[step // 2, i * PAD : i * PAD + EXT, :] = bits
    keep = lax.broadcasted_iota(jnp.int32, (PAD, NZ), 0) < EXT
    for i in range(EXT):
        turn_ref[HALF, i * PAD : (i + 1) * PAD, :] = mass_ref[i]
    for field, (place, planes) in enumerate(edge_layout(Y_LEFT)[0]):
        for y in range(EXT):
            line = pl.ds(y, PAD, stride=PAD)
            if field == 0:
                rows = own_ref[y] = jnp.where(keep, uy_ref[line, :], 0.0)
            elif field == 1:
                rows = y_mass_ref[y] = jnp.where(keep, turn_ref[HALF, line, :], 0.0)
            else:
                rows = y_bits_ref[field - 2, y] = jnp.where(keep, turn_ref[field - 2, line, :], 0.0)
            if y < planes:
                low_ref[place + y] = rows
            if y >= EXT - planes:
                high_ref[place + y - (EXT - planes)] = rows


def spread(carry, mass, uy, flags):
    edge = shape(edge_layout(Y_LEFT)[1], PAD, NZ)
    plane = shape(EXT, PAD, NZ)
    return pl.pallas_call(
        spread_kernel,
        in_specs=[VMEM] * 4,
        out_specs=[VMEM] * 6,
        out_shape=[shape(X_LEFT, EXT, PAD, NZ), plane, plane, shape(Y_LEFT, EXT, PAD, NZ), edge, edge],
        scratch_shapes=[pltpu.VMEM((HALF + 1, PAD * PAD, NZ), f32)],
        compiler_params=GRANT,
        name="spread",
    )(carry, mass, uy.reshape(PAD * PAD, NZ), flags)


def lower_start(parity_ref, step, brick_axis, halo):
    return lax.rem(parity_ref[step] + lax.axis_index(brick_axis) * EXT + halo, jnp.int32(2))


def first_kernel(
    carry_ref, own_ref, own_mass_ref, own_allow_ref, bits_ref, below_ref, above_ref,
    rows_ref, out_ref, next_ref, xlo_hbm, xhi_hbm, u_ref, mass_ref, allow_ref, xlo_ref, xhi_ref, sems,
):
    layout, edge_count = edge_layout(X_LEFT)
    edges = ((xlo_ref, xlo_hbm, 0), (xhi_ref, xhi_hbm, 1))
    for field, (place, planes) in enumerate(layout):
        for k in range(planes):
            for edge_ref, plane in ((xlo_ref, k), (xhi_ref, EXT - planes + k)):
                if field == 1:
                    edge_ref[place + k] = own_mass_ref[plane]
                elif field > 1:
                    edge_ref[place + k] = bits_ref[field - 2, plane]
    fixed, moved = pl.ds(X_LEFT, edge_count - X_LEFT), pl.ds(0, X_LEFT)
    sends = [pltpu.make_async_copy(src.at[fixed], dst.at[fixed], sems.at[k]) for src, dst, k in edges]
    for send in sends:
        send.start()
    for field, (all_ref, mine_ref) in enumerate(
        ((u_ref, own_ref), (mass_ref, own_mass_ref), (allow_ref, own_allow_ref))
    ):
        all_ref[0] = below_ref[field]
        all_ref[EXT + 1] = above_ref[field]
        for k in range(EXT):
            all_ref[1 + k] = mine_ref[k]
    start = whole(carry_ref, START_ROW)
    wide = jnp.broadcast_to(carry_ref[0:1, :], (PAD, NZ))
    for k in range((EXT + 1) // 2):
        plane = start + 2 * k
        low, high = u_ref[plane], u_ref[plane + 1]
        weight_low, weight_high = pair_weights(mass_ref[plane], mass_ref[plane + 1])
        allowed = jnp.maximum(allow_ref[plane], allow_ref[plane + 1])
        closing = jnp.maximum(low - high, 0.0)
        push = allowed * closing * jnp.tanh(wide * closing)
        u_ref[plane] = low - weight_low * push
        u_ref[plane + 1] = high + weight_high * push
    for k in range(EXT):
        next_ref[k] = u_ref[1 + k]
    for k in range(X_LEFT):
        xlo_ref[k] = u_ref[1 + k]
        xhi_ref[k] = u_ref[1 + EXT - X_LEFT + k]
    for src, dst, k in edges:
        sends.append(pltpu.make_async_copy(src.at[moved], dst.at[moved], sems.at[2 + k]))
        sends[-1].start()
    energy = jnp.zeros((PAD, NZ), f32)
    for k in range(EXT):
        u = next_ref[k]
        energy = energy + own_mass_ref[k] * u * u
    mine = fold(energy)
    half = NZ // 2
    lane = lax.broadcasted_iota(jnp.int32, (1, NZ), 1)
    local = carry_ref[2:3, :] + mine + carry_ref[4:5, :]
    number = carry_ref[5:6, :]
    local = jnp.where(lane < half, local + pltpu.roll(local, half, 1), number + pltpu.roll(number, half, 1))
    out_ref[...] = carry_ref[...]
    out_ref[3:4, :] = mine
    rows_ref[...] = jnp.broadcast_to(local, (DEVICES, NZ))
    for send in sends:
        send.wait()


def first(carry, own, mass, allow, bits, below, above):
    edge = (edge_layout(X_LEFT)[1], PAD, NZ)
    return pl.pallas_call(
        first_kernel,
        in_specs=[VMEM] * 7,
        out_specs=[VMEM] * 3 + [ANY] * 2,
        out_shape=[shape(DEVICES, NZ), shape(CARRY, NZ), shape(EXT, PAD, NZ), far(*edge), far(*edge)],
        scratch_shapes=[pltpu.VMEM((EXT + 2, PAD, NZ), f32)] * 3
        + [pltpu.VMEM(edge, f32)] * 2
        + [pltpu.SemaphoreType.DMA((4,))],
        compiler_params=GRANT,
        name="first",
    )(carry, own, mass, allow, bits, below, above)


def pair_weights(mass_low, mass_high):
    reduced = mass_low * mass_high / jnp.maximum(mass_low + mass_high, 1.0)
    return reduced / jnp.maximum(mass_low, 1.0), reduced / jnp.maximum(mass_high, 1.0)


def join_kernel(
    carry_ref, own_ref, mass_ref, own_bits_ref, below_ref, above_ref, u_ref, weight_ref, all_mass_ref, bits_ref, both_ref, *, left, first_step
):
    for field, (place, planes) in enumerate(edge_layout(left)[0]):
        for k in range(planes):
            low, high = below_ref[place + k], above_ref[place + k]
            below, above = left - planes + k, left + EXT + k
            if field == 0:
                u_ref[below], u_ref[above] = low, high
            elif field == 1:
                all_mass_ref[below], all_mass_ref[above] = low, high
            else:
                bits_ref[field - 2, below], bits_ref[field - 2, above] = low, high
        for k in range(left - planes):
            bits_ref[field - 2, k] = jnp.zeros((PAD, NZ), f32)
            bits_ref[field - 2, full_planes(left) - 1 - k] = jnp.zeros((PAD, NZ), f32)
    for k in range(EXT):
        u_ref[left + k] = own_ref[k]
        all_mass_ref[left + k] = mass_ref[k]
        for j in range(left):
            bits_ref[j, left + k] = own_bits_ref[j, k]
    for plane in range(full_planes(left) - 1):
        both_ref[0, plane], both_ref[1, plane] = pair_weights(all_mass_ref[plane], all_mass_ref[plane + 1])
    for j in range(left):
        start = whole(carry_ref, START_ROW + first_step + 2 * j)
        for k in range(pair_count(left)):
            plane = start + 2 * k
            allowed = jnp.maximum(bits_ref[j, plane], bits_ref[j, plane + 1])
            weight_ref[j, 0, k] = allowed * both_ref[0, plane]
            weight_ref[j, 1, k] = allowed * both_ref[1, plane]


def join(carry, own, mass, bits, below, above, left, first_step):
    def body(*refs):
        join_kernel(*refs, left=left, first_step=first_step)

    full, pairs = full_planes(left), pair_count(left)
    return pl.pallas_call(
        body,
        in_specs=[VMEM] * 6,
        out_specs=[VMEM] * 2,
        out_shape=[shape(full, PAD, NZ), shape(left, 2, pairs, PAD, NZ)],
        scratch_shapes=[
            pltpu.VMEM((full, PAD, NZ), f32),
            pltpu.VMEM((left, full, PAD, NZ), f32),
            pltpu.VMEM((2, full, PAD, NZ), f32),
        ],
        compiler_params=GRANT,
        name="join",
    )(carry, own, mass, bits, below, above)


def next_scale(received_ref, carry_ref, step):
    sums = jnp.sum(received_ref[...], axis=0, keepdims=True)
    scale = carry_ref[0:1, :]
    if step == 0:
        lane = lax.broadcasted_iota(jnp.int32, (1, NZ), 1)
        energy = jnp.sum(jnp.where(lane < NZ // 2, sums, 0.0), axis=1, keepdims=True)
        total = jnp.sum(jnp.where(lane < NZ // 2, 0.0, sums), axis=1, keepdims=True)
        total = jnp.broadcast_to(total, (1, NZ))
    else:
        energy = jnp.sum(sums, axis=1, keepdims=True)
        total = carry_ref[1:2, :]
    speed = scale * jnp.sqrt(jnp.broadcast_to(energy, (1, NZ)))
    factor = jnp.sqrt(carry_ref[HEAT_ROW + step : HEAT_ROW + step + 1, :] * total / (speed * speed + excess_coupling))
    return jnp.minimum(scale * factor, SCALE_CAP), total


def step_kernel(received_ref, carry_ref, u_in_ref, weight_ref, mass_ref, u_ref, rows_ref, out_ref, *, step, left):
    start = whole(carry_ref, START_ROW + step)
    scale, total = next_scale(received_ref, carry_ref, step - 1)
    wide = jnp.broadcast_to(scale, (PAD, NZ))
    turn = left - (STEPS + 1 - step) // 2
    u_ref[0] = u_in_ref[0]
    u_ref[full_planes(left) - 1] = u_in_ref[full_planes(left) - 1]
    for k in range(pair_count(left)):
        plane = start + 2 * k
        low, high = u_in_ref[plane], u_in_ref[plane + 1]
        closing = jnp.maximum(low - high, 0.0)
        push = closing * jnp.tanh(wide * closing)
        u_ref[plane] = low - weight_ref[turn, 0, k] * push
        u_ref[plane + 1] = high + weight_ref[turn, 1, k] * push
    energy = jnp.zeros((PAD, NZ), f32)
    for k in range(EXT):
        u = u_ref[left + k]
        energy = energy + mass_ref[k] * u * u
    mine = fold(energy)
    other = carry_ref[4:5, :] if step % 2 == 0 else carry_ref[3:4, :]
    out_ref[...] = carry_ref[...]
    out_ref[0:1, :] = scale
    out_ref[1:2, :] = total
    row = 3 if step % 2 == 0 else 4
    out_ref[row : row + 1, :] = mine
    rows_ref[...] = jnp.broadcast_to(carry_ref[2:3, :] + mine + other, (DEVICES, NZ))


def collide(step, received, carry, u, weight, mass):
    left, _ = place_of(step)

    def body(*refs):
        step_kernel(*refs, step=step, left=left)

    return pl.pallas_call(
        body,
        in_specs=[VMEM] * 5,
        out_specs=[VMEM] * 3,
        out_shape=[shape(full_planes(left), PAD, NZ), shape(DEVICES, NZ), shape(CARRY, NZ)],
        compiler_params=GRANT,
        name="collide",
    )(received, carry, u, weight, mass)


def turn_kernel(carry_ref, v_ref, ux_ref, uy_ref, uz_ref, spin_ref, w_hbm, w_ref, sems):
    shifts = [whole(carry_ref, SHIFT_ROW + step) for step in range(STEPS)]

    def plane(i, carry):
        real = jnp.ones((EXT, NZ), f32)
        parts = [jnp.zeros((EXT, NZ), f32)] * 3
        for step in range(STEPS):
            spin = pltpu.roll(spin_ref[step, i], shifts[step], 1)
            tangent = jnp.where((spin & 1) == 0, HALF_TAN, -HALF_TAN)
            on_x, on_y = spin < 2, spin < 4
            x, y, z = parts

            def pick(first, second, third):
                return tangent * jnp.where(on_x, first, jnp.where(on_y, second, third))

            real, parts = (
                real - pick(x, y, z),
                [x + pick(real, z, -y), y + pick(-z, real, x), z + pick(y, -x, real)],
            )
        x, y, z = parts
        unit = BIG * TURN_NORM
        xx, yy, zz, rr = x * x, y * y, z * z, real * real
        rows = [
            [(rr + xx) - (yy + zz), 2.0 * (x * y - real * z), 2.0 * (x * z + real * y)],
            [2.0 * (x * y + real * z), (rr + yy) - (xx + zz), 2.0 * (y * z - real * x)],
            [2.0 * (x * z - real * y), 2.0 * (y * z + real * x), (rr + zz) - (xx + yy)],
        ]
        rows = [[unit * value for value in row] for row in rows]
        mean = [mean_ref[i, 0:EXT, :] * (1.0 / BIG) for mean_ref in (ux_ref, uy_ref, uz_ref)]
        for slot in range(SLOTS):
            rest = [pltpu.roll(v_ref[member, slot, i], shifts[0], 1) - mean[member] for member in range(3)]
            for member in range(3):
                turned = rows[member][0] * rest[0] + rows[member][1] * rest[1] + rows[member][2] * rest[2]
                w_ref[member, slot, i] = turned
        send(i).start()
        return carry

    def send(i):
        part = pl.ds(i, 1)
        return pltpu.make_async_copy(w_ref.at[:, :, part], w_hbm.at[:, :, part], sems.at[i])

    lax.fori_loop(0, EXT, plane, 0, unroll=TURN_UNROLL)
    for i in range(EXT):
        send(i).wait()


def turn(carry, v, ux, uy, uz, spin):
    return pl.pallas_call(
        turn_kernel,
        in_specs=[VMEM] * 6,
        out_specs=ANY,
        out_shape=far(3, SLOTS, EXT, EXT, NZ),
        scratch_shapes=[pltpu.VMEM((3, SLOTS, EXT, EXT, NZ), f32), pltpu.SemaphoreType.DMA((EXT,))],
        compiler_params=GRANT,
        name="turn",
    )(carry, v, ux, uy, uz, spin)


def finish_kernel(received_ref, carry_ref, ux_ref, uy_ref, uz_ref, mass_ref, w_ref, v_hbm, v_ref, sems):
    scale, _ = next_scale(received_ref, carry_ref, STEPS - 1)
    wide = jnp.broadcast_to(scale, (EXT, NZ))
    sends = []
    for i in range(EXT):
        counts = mass_ref[i, 0:EXT, :]
        means = [
            ux_ref[X_LEFT + i, 0:EXT, :],
            uy_ref[pl.ds(Y_LEFT * PAD + i, EXT, stride=PAD), :],
            uz_ref[i, 0:EXT, :],
        ]
        for slot in range(SLOTS):
            live = counts > slot
            for member in range(3):
                v_ref[member, slot, i] = jnp.where(live, wide * (means[member] + w_ref[member, slot, i]), 0.0)
        if i % CHUNK == CHUNK - 1:
            part = pl.ds(i - (CHUNK - 1), CHUNK)
            sends.append(pltpu.make_async_copy(v_ref.at[:, :, part], v_hbm.at[:, :, part], sems.at[i // CHUNK]))
            sends[-1].start()
    for send in sends:
        send.wait()


def finish(received, carry, ux, uy, uz, mass, w):
    return pl.pallas_call(
        finish_kernel,
        in_specs=[VMEM] * 7,
        out_specs=ANY,
        out_shape=far(3, SLOTS, EXT, EXT, NZ),
        scratch_shapes=[pltpu.VMEM((3, SLOTS, EXT, EXT, NZ), f32), pltpu.SemaphoreType.DMA((EXT // CHUNK,))],
        compiler_params=GRANT,
        name="finish",
    )(received, carry, ux, uy.reshape(full_planes(Y_LEFT) * PAD, NZ), uz, mass, w)


def exchange(low_edge, high_edge, axis):
    count = lax.axis_size(axis)
    down = [(source, (source - 1) % count) for source in range(count)]
    up = [(source, (source + 1) % count) for source in range(count)]
    return lax.ppermute(low_edge, axis, down), lax.ppermute(high_edge, axis, up)


def sum_over_devices(rows):
    return lax.all_to_all(rows, ("bx", "by"), 0, 0, tiled=True)


def per_device(v, counts, spin, flags, parity, shifts, heat):
    ux, mass, allow, uy, uz, low, high, carry = prep(shifts, parity, heat, v, counts, flags)
    carry, v, spin, flags = lax.optimization_barrier((carry, v, spin, flags))
    mean_y = uy
    above, below = exchange(low, high, "bx")
    bits, uy, y_mass, y_bits, ylo, yhi = spread(carry, mass, uy, flags)
    y_above, y_below = exchange(ylo, yhi, "by")
    w = turn(carry, v, ux, mean_y, uz, spin)
    below, above, w = lax.optimization_barrier((below, above, w))
    rows, carry, ux, xlo, xhi = first(carry, ux, mass, allow, bits, below, above)
    received = sum_over_devices(rows)
    x_above, x_below = exchange(xlo, xhi, "bx")
    received, carry, uy = lax.optimization_barrier((received, carry, uy))
    uy, y_weights = join(carry, uy, y_mass, y_bits, y_below, y_above, Y_LEFT, 1)
    for step in range(1, STEPS):
        if step % 2 == 0:
            ux, rows, carry = collide(step, received, carry, ux, x_weights, mass)
        else:
            uy, rows, carry = collide(step, received, carry, uy, y_weights, y_mass)
        received = sum_over_devices(rows)
        if step == 1:
            received, carry, ux = lax.optimization_barrier((received, carry, ux))
            ux, x_weights = join(carry, ux, mass, bits, x_below, x_above, X_LEFT, 2)
    return finish(received, carry, ux, uy, uz, mass, w)


def solution(mesh):
    return jax.shard_map(
        per_device,
        mesh=mesh,
        in_specs=(
            P(None, None, "bx", "by", None),
            P("bx", "by", None),
            P(None, "bx", "by", None),
            P(None, "bx", "by", None),
            P(),
            P(),
            P(),
        ),
        out_specs=P(None, None, "bx", "by", None),
        check_vma=False,
    )
```
